32 devices in a mesh: seq: 8 (over y, x, core), head: 4 (over z).
Axes of the slice: x: 2, y: 2, z: 4, core: 2. Of those that a mesh axis runs over, the one named last changes fastest.
Arguments:
- queries: bfloat16 [1536, 2048], P('seq', 'head'), may hold values from -6 to 6, as said below
- keys: bfloat16 [1536, 256], P('seq'), may hold values from -6 to 6, as said below
- values: bfloat16 [1536, 256], P('seq'), may hold values from -6 to 6
- out_weight: bfloat16 [2048, 8192], P('head'), may hold values from -0.25 to 0.25
- doc_lengths: int32 [48], replicated, may hold values from 1 to 384, 1536 in all
- pair_ids: int32 [48], replicated, may hold values from 0 to 23, never falling along the last dimension, each value on 1 to 3 neighbouring positions
- block_plan: int32 [32], replicated, may hold values from 0 to 31, as said below
Outputs:
- projected: bfloat16 [1536, 8192], P(('seq', 'head'))
The draws below stay inside these ranges and needn't reach their ends.
Inputs may be any that keep to these rules, and one draw needn't show every extreme that they name: Entries of queries lie in the range given. Entries of keys lie in the range given. `doc_lengths`: the lengths sum to 1536. `pair_ids`: never falling; every pair 0 to 23 holds one to three consecutive documents. `block_plan`: A permutation of the 32 blocks of 48 tokens, numbered along the row. The 4 consecutive slots of one seq index hold blocks from 4 different seq indices, and the 4 blocks of one seq index go to 4 different seq indices.
All inputs are finite; a program needn't handle non-finite values.
Results may differ from the reference program's by a relative error of at most 0.015.
Values may be sent and summed in bfloat16 or wider, within the bound.
A program may use at most 64 MiB of HBM per device.

```python
import math
import jax
import jax.numpy as jnp
import numpy as np
from jax import lax

D = 8192
D_HEAD = 128
QH_DEV = 4
TOK_DEV = 192
NDOC = 48
NPAIR = 24
KV_HEADS = 2
Q_HEADS = 16
NB = 4
BLK = 48
NBLK = 32
SEQ_LEN = 1536
MAXDOC = 384


def paired_rows(key):
    query_key, keys_key = jax.random.split(jax.random.fold_in(key, 31), 2)
    query_width = Q_HEADS * D_HEAD
    key_width = KV_HEADS * D_HEAD
    query_vals = jnp.clip(jax.random.normal(query_key, (SEQ_LEN, query_width), jnp.float32), -6.0, 6.0)
    key_vals = jnp.clip(jax.random.normal(keys_key, (SEQ_LEN, key_width), jnp.float32), -6.0, 6.0)
    return (query_vals, key_vals)


def draw_queries(key, part):
    return paired_rows(key)[0].astype(jnp.bfloat16)


def draw_keys(key, part):
    return paired_rows(key)[1].astype(jnp.bfloat16)


def draw_block_plan(key, part):
    device_count = SEQ_LEN // TOK_DEV
    first_key, second_key, third_key, fourth_key = jax.random.split(jax.random.fold_in(key, 53), 4)
    offsets = jax.random.permutation(first_key, device_count)[:NB].astype(jnp.int32)
    outer = jax.random.permutation(second_key, device_count).astype(jnp.int32)
    inner = jax.random.permutation(third_key, device_count).astype(jnp.int32)
    local_order = jax.random.permutation(fourth_key, NB).astype(jnp.int32)
    outer_inverse = jnp.argsort(outer).astype(jnp.int32)
    inner_inverse = jnp.argsort(inner).astype(jnp.int32)
    shifted = (outer_inverse[:, None] - offsets[None, :]) % device_count
    source = inner_inverse[shifted]
    plan = source * NB + local_order[None, :]
    return plan.reshape(-1).astype(jnp.int32)


def block_levels(stream_key, shape, cuts, low, high):
    def one(axis_at, shards_of):
        draws = jax.random.uniform(jax.random.fold_in(jax.random.fold_in(stream_key, 6), axis_at), (shards_of,), jnp.float32, low / len(cuts), high / len(cuts))
        return jnp.repeat(jnp.exp(draws), shape[axis_at] // shards_of).reshape((-1,) + (1,) * (len(shape) - axis_at - 1))

    level = one(*cuts[0])
    for cut in cuts[1:]:
        level = level * one(*cut)
    return level


def profile(amount, total, most, lean):
    weights = [(1 << 20) // math.isqrt(rank ** lean) + 1 for rank in range(2, amount + 1)]
    surplus, holding = total - most - (amount - 1), [1] * (amount - 1)
    while surplus > 0:
        movable = [i for i in range(amount - 1) if holding[i] < most]
        mass, budget = sum([weights[i] for i in movable]), surplus
        for i in movable:
            more = min(most - holding[i], max(1, budget * weights[i] // mass), surplus)
            holding[i] = holding[i] + more
            surplus = surplus - more
    return np.array([most] + holding)


def ragged(stream_key, count, total, bound, slope):
    if count == 2:
        one = jax.random.randint(stream_key, (), max(1, total - bound), min(bound, total - 1) + 1)
        return jnp.stack([one, total - one])
    lengths = jnp.asarray(profile(count, total, bound, slope), jnp.int32)
    pairs = (count - 1) // 2
    donor, receiver = lengths[1:1 + 2 * pairs:2], lengths[2:2 + 2 * pairs:2]
    room = jnp.minimum(donor - 1, bound - receiver)
    passed = jax.random.randint(jax.random.fold_in(stream_key, 1), (pairs,), 0, 1 << 20) % (room + 1)
    lengths = lengths.at[1:1 + 2 * pairs:2].set(donor - passed).at[2:2 + 2 * pairs:2].set(receiver + passed)
    return lengths[jax.random.permutation(jax.random.fold_in(stream_key, 2), count)]


def normal_values(own_key, extent, deviation, reach, cuts=(), kind=jnp.bfloat16):
    array = deviation * jax.random.normal(own_key, extent, jnp.float32)
    if cuts:
        array = array * block_levels(own_key, extent, cuts, -0.22, 0.18)
    return jnp.clip(array, -reach, reach).astype(kind)


def setup_inputs(seed: int = 0) -> dict:
    seeds = jax.random.split(jax.random.key(seed), 8)
    queries = draw_queries(jax.random.fold_in(seeds[7], 71), 0)
    keys = draw_keys(jax.random.fold_in(seeds[7], 71), 0)
    values = normal_values(seeds[2], (SEQ_LEN, KV_HEADS * D_HEAD), 1.0, 6.0, ((0, 8),))
    out_weight = normal_values(seeds[3], (Q_HEADS * D_HEAD, D), (QH_DEV * D_HEAD) ** -0.5, 0.25, ((0, 4),))
    doc_lengths = ragged(seeds[4], NDOC, SEQ_LEN, MAXDOC, 2).astype(jnp.int32)
    pair_ids = jnp.searchsorted(jnp.cumsum(ragged(seeds[5], NPAIR, NDOC, 3, 0)), jnp.arange(NDOC), side="right").astype(jnp.int32)
    block_plan = draw_block_plan(jax.random.fold_in(seeds[7], 71), 0)
    return {"queries": queries, "keys": keys, "values": values, "out_weight": out_weight, "doc_lengths": doc_lengths, "pair_ids": pair_ids, "block_plan": block_plan}


NEGATIVE = -1e+30

def token_docs(positions, doc_lengths):
    doc_ends = jnp.cumsum(doc_lengths)
    return lax.optimization_barrier(jnp.sum((doc_ends[None, :] <= positions[:, None]).astype(jnp.int32), axis=1))

def pair_firsts(docs, pair_ids):
    doc_range = jnp.arange(pair_ids.shape[0], dtype=jnp.int32)
    own_pair = lax.optimization_barrier(jnp.sum(jnp.where(docs[:, None] == doc_range[None, :], pair_ids[None, :], 0), axis=1))
    return lax.optimization_barrier(jnp.sum((pair_ids[None, :] < own_pair[:, None]).astype(jnp.int32), axis=1))

def reference(queries, keys, values, out_weight, doc_lengths, pair_ids, block_plan):
    positions = jnp.arange(SEQ_LEN, dtype=jnp.int32)
    docs_all = token_docs(positions, doc_lengths)
    firsts_all = pair_firsts(docs_all, pair_ids)
    scale = 1.0 / math.sqrt(D_HEAD)
    query_block = 4 * TOK_DEV
    block_total = SEQ_LEN // query_block
    group_total = Q_HEADS // QH_DEV

    def one_group(group_index):
        kv_index = group_index // 2
        key_rows = lax.dynamic_slice_in_dim(keys, (kv_index * D_HEAD).astype(jnp.int32), D_HEAD, 1).astype(jnp.float32)
        value_rows = lax.dynamic_slice_in_dim(values, (kv_index * D_HEAD).astype(jnp.int32), D_HEAD, 1).astype(jnp.float32)
        group_queries = lax.dynamic_slice_in_dim(queries, (group_index * QH_DEV * D_HEAD).astype(jnp.int32), QH_DEV * D_HEAD, 1)

        def one_block(block_index):
            start_row = (block_index * query_block).astype(jnp.int32)
            query_rows = lax.dynamic_slice_in_dim(group_queries, start_row, query_block, 0)
            query_rows = query_rows.astype(jnp.float32).reshape(query_block, QH_DEV, D_HEAD)
            row_pos = lax.dynamic_slice_in_dim(positions, start_row, query_block, 0)
            row_docs = lax.dynamic_slice_in_dim(docs_all, start_row, query_block, 0)
            row_firsts = lax.dynamic_slice_in_dim(firsts_all, start_row, query_block, 0)
            allowed = (positions[None, :] <= row_pos[:, None]) & ((docs_all[None, :] == row_docs[:, None]) | (docs_all[None, :] == row_firsts[:, None]))
            scores = jnp.einsum('qhd,kd->hqk', query_rows, key_rows) * scale
            row_max = lax.optimization_barrier(jnp.max(jnp.where(allowed[None], scores, NEGATIVE), axis=2))
            weights = jnp.where(allowed[None], jnp.exp(scores - row_max[:, :, None]), 0.0)
            denominator = lax.optimization_barrier(jnp.sum(weights, axis=2))
            rounded = lax.optimization_barrier(weights.astype(jnp.bfloat16)).astype(jnp.float32)
            combined = jnp.einsum('hqk,kd->hqd', rounded, value_rows) / denominator[:, :, None]
            return combined.transpose(1, 0, 2).reshape(query_block, QH_DEV * D_HEAD).astype(jnp.bfloat16)
        outputs = lax.map(one_block, jnp.arange(block_total, dtype=jnp.int32))
        return outputs.reshape(SEQ_LEN, QH_DEV * D_HEAD)
    grouped = lax.map(one_group, jnp.arange(group_total, dtype=jnp.int32))
    attended = grouped.transpose(1, 0, 2).reshape(SEQ_LEN, group_total * QH_DEV * D_HEAD)
    planned = attended.reshape(NBLK, BLK, group_total * QH_DEV * D_HEAD)[block_plan]
    planned = planned.reshape(SEQ_LEN, group_total, QH_DEV * D_HEAD)
    weight_groups = out_weight.reshape(group_total, QH_DEV * D_HEAD, D)

    def add_group(running_total, group_index):
        group_rows = lax.dynamic_index_in_dim(planned, group_index, 1, False)
        group_weight = lax.dynamic_index_in_dim(weight_groups, group_index, 0, False)
        partial_term = jnp.dot(group_rows, group_weight, preferred_element_type=jnp.float32).astype(jnp.bfloat16)
        return (running_total + lax.optimization_barrier(partial_term).astype(jnp.float32), None)
    summed, unused_out = lax.scan(add_group, jnp.zeros((SEQ_LEN, D), jnp.float32), jnp.arange(group_total, dtype=jnp.int32))
    return summed.astype(jnp.bfloat16)
```

```python
import functools
import math

import jax
import jax.numpy as jnp
from jax import lax
from jax.experimental import pallas as pl
from jax.experimental.pallas import tpu as pltpu
from jax.sharding import PartitionSpec as P

D_HEAD = 128


NEGATIVE = -1e30


def token_docs(positions, doc_lengths):
    doc_ends = jnp.cumsum(doc_lengths)
    return jnp.sum((doc_ends[None, :] <= positions[:, None]).astype(jnp.int32), axis=1)


def pair_firsts(docs, pair_ids):
    doc_range = jnp.arange(pair_ids.shape[0], dtype=jnp.int32)
    own_pair = jnp.sum(jnp.where(docs[:, None] == doc_range[None, :], pair_ids[None, :], 0), axis=1)
    return jnp.sum((pair_ids[None, :] < own_pair[:, None]).astype(jnp.int32), axis=1)


def largest_divisor(total_rows, ceiling):
    return max(
        (
            candidate
            for candidate in range(1, min(total_rows, ceiling) + 1)
            if total_rows % candidate == 0
        )
    )


def attend(query_rows, positions, keys, values, doc_lengths, pair_ids):
    head_size = keys.shape[1]
    token_count = query_rows.shape[0]
    query_heads = query_rows.shape[1] // head_size
    shaped_queries = query_rows.reshape(token_count, query_heads, head_size)
    query_docs = token_docs(positions, doc_lengths)
    query_firsts = pair_firsts(query_docs, pair_ids)
    doc_range = jnp.arange(doc_lengths.shape[0], dtype=jnp.int32)
    pair_begin = jnp.sum(
        jnp.where(doc_range[None, :] < query_firsts[:, None], doc_lengths[None, :], 0), axis=1
    )
    lowest = jnp.min(pair_begin)
    highest = jnp.max(positions)
    scale = 1.0 / math.sqrt(head_size)

    def update(softmax_state, key_block, value_block, block_start):
        key_pos = block_start + jnp.arange(key_block.shape[0], dtype=jnp.int32)
        needed = (block_start <= highest) & (block_start + key_block.shape[0] > lowest)

        def compute(current):
            running_max, denominator, weighted = current
            key_docs = token_docs(key_pos, doc_lengths)
            allowed = (key_pos[None, :] <= positions[:, None]) & (
                (key_docs[None, :] == query_docs[:, None])
                | (key_docs[None, :] == query_firsts[:, None])
            )
            scores = (
                jnp.einsum(
                    "qhd,kd->hqk", shaped_queries, key_block, preferred_element_type=jnp.float32
                )
                * scale
            )
            newest = jnp.maximum(
                running_max, jnp.max(jnp.where(allowed[None], scores, NEGATIVE), axis=2)
            )
            weights = jnp.where(allowed[None], jnp.exp(scores - newest[:, :, None]), 0.0)
            factor = jnp.exp(running_max - newest)
            denominator = denominator * factor + jnp.sum(weights, axis=2)
            weighted = weighted * factor[:, :, None] + jnp.einsum(
                "hqk,kd->hqd",
                weights.astype(jnp.bfloat16),
                value_block,
                preferred_element_type=jnp.float32,
            )
            return (newest, denominator, weighted)

        def unchanged(current):
            return current

        return lax.cond(needed, compute, unchanged, softmax_state)

    initial = (
        jnp.full((query_heads, token_count), NEGATIVE, jnp.float32),
        jnp.zeros((query_heads, token_count), jnp.float32),
        jnp.zeros((query_heads, token_count, head_size), jnp.float32),
    )
    key_rows = lax.all_gather(keys, "seq", axis=0, tiled=True)
    value_rows = lax.all_gather(values, "seq", axis=0, tiled=True)
    row_total = key_rows.shape[0]
    block_rows = largest_divisor(row_total, 1024)
    block_count = row_total // block_rows
    stacked = (
        key_rows.reshape(block_count, block_rows, head_size),
        value_rows.reshape(block_count, block_rows, head_size),
        jnp.int32(0) + block_rows * jnp.arange(block_count, dtype=jnp.int32),
    )

    def advance(carried, block_item):
        return (update(carried, block_item[0], block_item[1], block_item[2]), None)

    result_state, unused_out = lax.scan(advance, initial, stacked)
    running_max, denominator, weighted = result_state
    attended = weighted / denominator[:, :, None]
    return (
        attended.transpose(1, 0, 2)
        .reshape(token_count, query_heads * head_size)
        .astype(jnp.bfloat16)
    )


def on_device(queries, keys, values, out_weight, doc_lengths, pair_ids, block_plan):
    seq_count = lax.axis_size("seq")
    my_seq = lax.axis_index("seq")
    shared_head = lax.axis_index("head") // 2
    key_rows = lax.dynamic_slice_in_dim(keys, shared_head * D_HEAD, D_HEAD, 1)
    value_rows = lax.dynamic_slice_in_dim(values, shared_head * D_HEAD, D_HEAD, 1)
    slots_here = seq_count // 2
    tok_rows = queries.shape[0]
    row_width = queries.shape[1]
    block_rows = tok_rows // slots_here
    slot_total = block_plan.shape[0]
    local_ids = my_seq * slots_here + jnp.arange(slots_here, dtype=jnp.int32)
    plan_rows = lax.dynamic_slice_in_dim(block_plan, my_seq * slots_here, slots_here, 0)
    planned_pos = (
        plan_rows[:, None] * block_rows + jnp.arange(block_rows, dtype=jnp.int32)[None, :]
    ).reshape(-1)
    slot_range = jnp.arange(slot_total, dtype=jnp.int32)
    target_slot = jnp.sum(
        jnp.where(block_plan[None, :] == local_ids[:, None], slot_range[None, :], 0), axis=1
    )
    device_range = jnp.arange(seq_count, dtype=jnp.int32)
    send_table = ((target_slot // slots_here)[:, None] == device_range[None, :]).astype(
        jnp.bfloat16
    )
    take_table = ((plan_rows // slots_here)[:, None] == device_range[None, :]).astype(jnp.bfloat16)
    blocked = queries.reshape(slots_here, block_rows, row_width)
    arrived = lax.all_to_all(
        jnp.einsum("bn,bkw->nkw", send_table, blocked, preferred_element_type=jnp.float32).astype(
            jnp.bfloat16
        ),
        "seq",
        split_axis=0,
        concat_axis=0,
        tiled=True,
    )
    chosen = jnp.einsum("bn,nkw->bkw", take_table, arrived, preferred_element_type=jnp.float32)
    attended = attend(
        chosen.astype(jnp.bfloat16).reshape(tok_rows, row_width),
        planned_pos,
        key_rows,
        value_rows,
        doc_lengths,
        pair_ids,
    )
    return lax.psum_scatter(
        jnp.dot(attended, out_weight, preferred_element_type=jnp.float32).astype(jnp.bfloat16),
        "head",
        scatter_dimension=0,
        tiled=True,
    )


FAR = 1e9
AHEAD = 3
EARLY = 4


def pick_tiles(width):
    return max(c for c in (1, 2, 4, 8, 16) if width % (c * 128) == 0)


def fused_kernel(
    seq_count,
    head_count,
    queries_ref,
    keys_ref,
    values_ref,
    weight_hbm,
    pairs_ref,
    lens_ref,
    plan_ref,
    out_ref,
    w_own,
    w_far,
    kv_all,
    q_send,
    q_recv,
    q_heads,
    bias,
    attended,
    sent,
    arrived,
    final,
    own_sem,
    kv_sems,
    q_sems,
    qz_sems,
    wz_sems,
    wr_sems,
    a_sems,
    b_sems,
    f_sems,
):
    me = lax.axis_index("seq")
    rank = lax.axis_index("head")
    core = lax.rem(me, 2)
    partner = me + 1 - 2 * core
    along_x = me + 2 - 4 * lax.rem(me // 2, 2)
    along_y = lax.rem(me + seq_count // 2, seq_count)
    first = jnp.where(core == 0, along_x, along_y)
    second = jnp.where(core == 0, along_y, along_x)
    low = rank < head_count // 2
    inner = (rank > 0) & (rank < head_count - 1)
    mate = rank + 1 - 2 * lax.rem(rank, 2)
    across = head_count - 1 - rank
    slots, block_rows, width = queries_ref.shape
    tokens = slots * block_rows
    seq_len = seq_count * tokens
    heads = width // D_HEAD
    shared = head_count // (keys_ref.shape[1] // D_HEAD)
    tiles, rows_all, tile = sent.shape
    half = tiles * tile
    share = width // (seq_count // 2)

    def slot_at(place):
        at = (head_count - 1, head_count // 2, 0, 1)[place]
        return jnp.where(low, at, head_count - 1 - at)

    def share_rows(device):
        return pl.ds(pl.multiple_of((device // 2) * share, share), share)

    def tile_cols(at):
        return pl.ds(pl.multiple_of(at * tile, tile), tile)

    def out_cols(side, at):
        return pl.ds(pl.multiple_of(side * half + at * tile, tile), tile)

    own_copy = pltpu.make_async_copy(
        weight_hbm.at[:, pl.ds(pl.multiple_of(core * half, half), half)], w_own, own_sem
    )

    barrier = pltpu.get_barrier_semaphore()
    for step in range(1, seq_count):
        pl.semaphore_signal(barrier, inc=1, device_id={"seq": lax.rem(me + step, seq_count)})

    @pl.when(rank > 0)
    def _():
        pl.semaphore_signal(barrier, inc=1, device_id={"head": rank - 1})
        pl.semaphore_signal(barrier, inc=1, device_id={"seq": partner, "head": rank - 1})

    @pl.when(rank < head_count - 1)
    def _():
        pl.semaphore_signal(barrier, inc=1, device_id={"head": rank + 1})
        pl.semaphore_signal(barrier, inc=1, device_id={"seq": partner, "head": rank + 1})

    @pl.when(inner)
    def _():
        own_copy.start()
        kv_col = pl.ds(pl.multiple_of((rank // shared) * D_HEAD, D_HEAD), D_HEAD)
        mine = pl.ds(pl.multiple_of(me * tokens, tokens), tokens)
        kv_all[0, mine] = keys_ref[:, kv_col]
        kv_all[1, mine] = values_ref[:, kv_col]

    for other in range(seq_count):
        local = jnp.int32(0)
        for slot in range(slots):
            offset = plan_ref[other * slots + slot] - me * slots
            local = local + jnp.where((offset >= 0) & (offset < slots), offset, 0)
        q_send[other] = queries_ref[local]
    q_recv[me] = q_send[me]

    edges = jnp.where(rank > 0, 2, 0) + jnp.where(rank < head_count - 1, 2, 0)
    pl.semaphore_wait(barrier, seq_count - 1 + edges)

    def kv_copy(peer, slot, sender):
        rows = pl.ds(pl.multiple_of(slot * tokens, tokens), tokens)
        return pltpu.make_async_remote_copy(
            src_ref=kv_all.at[:, rows],
            dst_ref=kv_all.at[:, rows],
            send_sem=kv_sems.at[0, sender],
            recv_sem=kv_sems.at[1, slot],
            device_id={"seq": peer},
        )

    def q_copy(peer, slot):
        return pltpu.make_async_remote_copy(
            src_ref=q_send.at[peer],
            dst_ref=q_recv.at[slot],
            send_sem=q_sems.at[0, peer],
            recv_sem=q_sems.at[1, slot],
            device_id={"seq": peer},
        )

    def qz_copy(part):
        return pltpu.make_async_remote_copy(
            src_ref=q_heads.at[0, pl.ds(part * 2, 2)],
            dst_ref=q_heads.at[1, pl.ds(part * 2, 2)],
            send_sem=qz_sems.at[0, part],
            recv_sem=qz_sems.at[1, part],
            device_id={"head": mate},
        )

    def wz_copy(at):
        return pltpu.make_async_remote_copy(
            src_ref=weight_hbm.at[share_rows(me), out_cols(core, at)],
            dst_ref=w_far.at[share_rows(me), tile_cols(at)],
            send_sem=wz_sems.at[0, at],
            recv_sem=wz_sems.at[1, at],
            device_id={"head": mate},
        )

    def relay(kind, source, peer, at):
        return pltpu.make_async_remote_copy(
            src_ref=w_far.at[share_rows(source), tile_cols(at)],
            dst_ref=w_far.at[share_rows(source), tile_cols(at)],
            send_sem=wr_sems.at[0, kind, at],
            recv_sem=wr_sems.at[1, kind, at],
            device_id={"seq": peer},
        )

    def a_copy(place, side):
        return pltpu.make_async_remote_copy(
            src_ref=attended.at[place, side],
            dst_ref=attended.at[place, side],
            send_sem=a_sems.at[0, place],
            recv_sem=a_sems.at[1, place],
            device_id={"seq": partner},
        )

    def b_copy(at):
        return pltpu.make_async_remote_copy(
            src_ref=sent.at[at],
            dst_ref=arrived.at[at],
            send_sem=b_sems.at[0, at],
            recv_sem=b_sems.at[1, at],
            device_id={"head": across},
        )

    def edge_copy(side, at, sender):
        return pltpu.make_async_remote_copy(
            src_ref=final.at[at, pl.ds(side * block_rows, block_rows)],
            dst_ref=out_ref.at[:, out_cols(sender, at)],
            send_sem=f_sems.at[0, side, at],
            recv_sem=f_sems.at[1, sender, at],
            device_id={"seq": me - core + side, "head": mate},
        )

    def mate_copy(at, sender):
        rows = pl.ds(
            pl.multiple_of((3 - sender) * block_rows, block_rows), block_rows
        )
        return pltpu.make_async_remote_copy(
            src_ref=final.at[at, rows],
            dst_ref=out_ref.at[:, out_cols(sender, at)],
            send_sem=f_sems.at[0, 2, at],
            recv_sem=f_sems.at[1, 2, at],
            device_id={"seq": partner},
        )

    @pl.when(inner)
    def _():
        for step in range(2, seq_count, 2):
            peer = lax.rem(me + step, seq_count)
            kv_copy(peer, me, peer).start()
        kv_copy(partner, me, me).start()

    @pl.when(jnp.logical_not(inner))
    def _():
        for at in range(min(EARLY, tiles)):
            wz_copy(at).start()

    for step in range(1, seq_count):
        peer = lax.rem(me + step, seq_count)
        q_copy(peer, me).start()

    def gather_queries():
        for step in range(1, seq_count):
            source = lax.rem(me + seq_count - step, seq_count)
            q_copy(source, source).wait_recv()
        for place in range(slots):
            block = q_recv[plan_ref[me * slots + slot_at(place)] // slots]
            for head in range(heads):
                q_heads[0, place, head * block_rows : (head + 1) * block_rows, :] = block[
                    :, head * D_HEAD : (head + 1) * D_HEAD
                ]

    @pl.when(jnp.logical_not(inner))
    def _():
        gather_queries()
        qz_copy(0).start()
        qz_copy(1).start()
        for at in range(min(EARLY, tiles), tiles):
            wz_copy(at).start()

        def collect(at, carry):
            edge_copy(0, at, 0).wait_recv()
            edge_copy(1, at, 1).wait_recv()
            wz_copy(at).wait_send()
            return carry

        lax.fori_loop(0, tiles, collect, 0)
        qz_copy(0).wait_send()
        qz_copy(1).wait_send()

    @pl.when(inner)
    def _():
        row = lax.broadcasted_iota(jnp.int32, (tokens, 1), 0)
        position = row
        for place in range(slots):
            shift = (plan_ref[me * slots + slot_at(place)] - place) * block_rows
            here = (row >= place * block_rows) & (row < (place + 1) * block_rows)
            position = position + jnp.where(here, shift, 0)
        position = position.astype(jnp.float32)
        docs = pairs_ref.shape[1]
        doc_at = lax.broadcasted_iota(jnp.int32, (1, docs), 1)
        starts = jnp.zeros((1, docs), jnp.int32)
        ends = jnp.zeros((1, docs), jnp.int32)
        running = jnp.int32(0)
        for doc in range(docs):
            starts = jnp.where(doc_at == doc, running, starts)
            running = running + lens_ref[doc]
            ends = jnp.where(doc_at == doc, running, ends)
        starts = starts.astype(jnp.float32)
        ends = ends.astype(jnp.float32)
        pairs = pairs_ref[...].astype(jnp.float32)
        begun = starts <= position
        own_start = jnp.max(jnp.where(begun, starts, 0.0), axis=1, keepdims=True)
        own_pair = jnp.max(jnp.where(begun, pairs, 0.0), axis=1, keepdims=True)
        same = pairs == own_pair
        first_start = jnp.min(jnp.where(same, starts, FAR), axis=1, keepdims=True)
        first_end = jnp.min(jnp.where(same, ends, FAR), axis=1, keepdims=True)
        key_width = 2 * D_HEAD
        parts = seq_len // key_width
        for part in range(parts):
            key_pos = (
                lax.broadcasted_iota(jnp.int32, (tokens, key_width), 1) + part * key_width
            ).astype(jnp.float32)
            seen = (key_pos <= position) & (
                (key_pos >= own_start) | ((key_pos >= first_start) & (key_pos < first_end))
            )
            bias[part] = jnp.where(seen, 0.0, NEGATIVE)

        for step in range(2, seq_count, 2):
            source = lax.rem(me + seq_count - step, seq_count)
            kv_copy(partner, source, source).wait_recv()
            kv_copy(partner, source, seq_count + source).start()

        def pass_on(at):
            wz_copy(at).wait_recv()
            relay(0, me, first, at).start()
            relay(1, me, second, at).start()

        def pass_far(at):
            relay(0, first, first, at).wait_recv()
            relay(2, first, second, at).start()

        def complete(at):
            relay(1, second, second, at).wait_recv()
            relay(2, lax.rem(first + second - me + seq_count, seq_count), second, at).wait_recv()

        pass_on(0)
        gather_queries()
        pass_on(1)
        kv_copy(partner, partner, me).wait_recv()
        for step in range(2, seq_count, 2):
            source = lax.rem(partner + seq_count - step, seq_count)
            kv_copy(partner, source, source).wait_recv()

        scale = math.log2(math.e) / math.sqrt(D_HEAD)

        def unit(group, place):
            rows_q = q_heads[group, place]
            rows_at = pl.ds(pl.multiple_of(place * block_rows, block_rows), block_rows)
            scores = []
            for part in range(parts):
                scores.append(
                    lax.dot_general(
                        rows_q,
                        kv_all[0, part * key_width : (part + 1) * key_width],
                        (((1,), (1,)), ((), ())),
                        preferred_element_type=jnp.float32,
                    )
                    * scale
                    + jnp.concatenate([bias[part, rows_at, :]] * heads, axis=0)
                )
            top = functools.reduce(jnp.maximum, scores)
            top = jnp.max(top, axis=1, keepdims=True)
            total = jnp.zeros((heads * block_rows, key_width), jnp.float32)
            summed = jnp.zeros((heads * block_rows, D_HEAD), jnp.float32)
            for part in range(parts):
                weights = jnp.exp2(scores[part] - top)
                total = total + weights
                summed = summed + jnp.dot(
                    weights.astype(jnp.bfloat16),
                    kv_all[1, part * key_width : (part + 1) * key_width],
                    preferred_element_type=jnp.float32,
                )
            total = jnp.sum(total, axis=1, keepdims=True)
            result = (summed / total).astype(jnp.bfloat16)
            for head in range(heads):
                at = (group * heads + head) * D_HEAD
                attended[place, core, :, at : at + D_HEAD] = result[
                    head * block_rows : (head + 1) * block_rows
                ]

        def own_unit(place, carry):
            unit(0, place)

            @pl.when(place < 2)
            def _():
                pass_on(place + 2)

            pass_far(place)
            return carry

        lax.fori_loop(0, slots, own_unit, 0)

        def far_unit(place, carry):
            unit(1, place)
            a_copy(place, core).start()
            return carry

        def term(place, at):
            rows_a = attended[place : place + 2].reshape(rows_all, 2 * width)
            return jnp.dot(
                rows_a[:, :width], w_own[:, tile_cols(at)], preferred_element_type=jnp.float32
            ) + jnp.dot(
                rows_a[:, width:], w_far[:, tile_cols(at)], preferred_element_type=jnp.float32
            )

        def send_term(at):
            complete(at)
            sent[at] = term(0, at).astype(jnp.bfloat16)
            b_copy(at).start()

        def keep_term(at):
            mixed = term(2, at)
            b_copy(at).wait_recv()
            final[at] = (mixed + arrived[at].astype(jnp.float32)).astype(jnp.bfloat16)
            edge_copy(0, at, core).start()
            edge_copy(1, at, core).start()
            mate_copy(at, core).start()
            rows = pl.ds(pl.multiple_of((2 + core) * block_rows, block_rows), block_rows)
            out_ref[:, out_cols(core, at)] = final[at, rows]

        qz_copy(0).wait_recv()
        lax.fori_loop(0, 2, far_unit, 0)
        own_copy.wait()
        pass_on(4)
        a_copy(0, 1 - core).wait_recv()
        a_copy(1, 1 - core).wait_recv()
        send_term(0)
        pass_far(4)
        send_term(1)
        qz_copy(1).wait_recv()
        lax.fori_loop(2, slots, far_unit, 0)
        pass_on(5)
        send_term(2)
        a_copy(2, 1 - core).wait_recv()
        a_copy(3, 1 - core).wait_recv()

        def advance(at, carry):
            @pl.when(at + 6 < tiles)
            def _():
                pass_on(at + 6)

            @pl.when(at + 5 < tiles)
            def _():
                pass_far(at + 5)

            @pl.when(at + AHEAD < tiles)
            def _():
                send_term(at + AHEAD)

            keep_term(at)
            return carry

        lax.fori_loop(0, tiles, advance, 0)

        def drain(at, carry):
            mate_copy(at, 1 - core).wait_recv()
            mate_copy(at, core).wait_send()
            edge_copy(0, at, core).wait_send()
            edge_copy(1, at, core).wait_send()
            b_copy(at).wait_send()
            relay(0, me, first, at).wait_send()
            relay(1, me, second, at).wait_send()
            relay(2, first, second, at).wait_send()
            return carry

        lax.fori_loop(0, tiles, drain, 0)
        for place in range(slots):
            a_copy(place, core).wait_send()
        for step in range(2, seq_count, 2):
            peer = lax.rem(me + step, seq_count)
            kv_copy(peer, me, peer).wait_send()
            kv_copy(partner, peer, seq_count + peer).wait_send()
        kv_copy(partner, me, me).wait_send()

    for step in range(1, seq_count):
        peer = lax.rem(me + step, seq_count)
        q_copy(peer, me).wait_send()


def fused_device(queries, keys, values, out_weight, doc_lengths, pair_ids, block_plan):
    seq_count = lax.axis_size("seq")
    head_count = lax.axis_size("head")
    tokens, width = queries.shape
    slots = block_plan.shape[0] // seq_count
    block_rows = tokens // slots
    out_width = out_weight.shape[1]
    half_width = out_width // 2
    tiles = pick_tiles(half_width)
    tile = half_width // tiles
    half = jnp.bfloat16
    flow = pltpu.VMEM((tiles, 4 * block_rows, tile), half)
    weights = pltpu.VMEM((width, half_width), half)
    in_vmem = pl.BlockSpec(memory_space=pltpu.VMEM)
    in_smem = pl.BlockSpec(memory_space=pltpu.SMEM)
    dma = pltpu.SemaphoreType.DMA
    return pl.pallas_call(
        functools.partial(fused_kernel, seq_count, head_count),
        out_shape=jax.ShapeDtypeStruct((block_rows, out_width), half),
        in_specs=[
            in_vmem,
            in_vmem,
            in_vmem,
            pl.BlockSpec(memory_space=pl.ANY),
            in_vmem,
            in_smem,
            in_smem,
        ],
        out_specs=in_vmem,
        scratch_shapes=[
            weights,
            weights,
            pltpu.VMEM((2, seq_count * tokens, D_HEAD), half),
            pltpu.VMEM((seq_count, block_rows, width), half),
            pltpu.VMEM((seq_count, block_rows, width), half),
            pltpu.VMEM((2, slots, width // D_HEAD * block_rows, D_HEAD), half),
            pltpu.VMEM(
                (seq_count * tokens // (2 * D_HEAD), tokens, 2 * D_HEAD), jnp.float32
            ),
            pltpu.VMEM((slots, 2, block_rows, 2 * width), half),
            flow,
            flow,
            flow,
            dma,
            dma((2, 2 * seq_count)),
            dma((2, seq_count)),
            dma((2, 2)),
            dma((2, tiles)),
            dma((2, 3, tiles)),
            dma((2, slots)),
            dma((2, tiles)),
            dma((2, 3, tiles)),
        ],
        compiler_params=pltpu.CompilerParams(
            collective_id=0, has_side_effects=True, vmem_limit_bytes=60000 * 1024
        ),
    )(
        queries.reshape(slots, block_rows, width),
        keys,
        values,
        out_weight,
        pair_ids[None],
        doc_lengths,
        block_plan,
    )


def pick_device(queries, keys, values, out_weight, doc_lengths, pair_ids, block_plan):
    seq_count = lax.axis_size("seq")
    head_count = lax.axis_size("head")
    tokens, width = queries.shape
    out_width = out_weight.shape[1]
    block_rows = tokens * seq_count // block_plan.shape[0]
    fits = seq_count * tokens * tokens * 4 <= 4 * 1024 * 1024
    shape = head_count == 4 and seq_count == 8 and keys.shape[1] == 2 * D_HEAD
    square = block_rows * head_count == tokens and block_rows % 16 == 0
    even = seq_count * tokens % (2 * D_HEAD) == 0 and width % 64 == 0
    wide = out_width % 2 == 0 and out_width // 2 % (16 * 128) == 0
    run = fused_device if fits and shape and square and even and wide else on_device
    return run(queries, keys, values, out_weight, doc_lengths, pair_ids, block_plan)


def solution(mesh):
    return jax.shard_map(
        pick_device,
        mesh=mesh,
        in_specs=(P("seq", "head"), P("seq", None), P("seq", None), P("head", None), P(), P(), P()),
        out_specs=P(("seq", "head"), None),
        check_vma=False,
    )
```

```python
import functools
import math

import jax
import jax.numpy as jnp
from jax import lax
from jax.experimental import pallas as pl
from jax.experimental.pallas import tpu as pltpu
from jax.sharding import PartitionSpec as P

D_HEAD = 128


NEGATIVE = -1e30


def token_docs(positions, doc_lengths):
    doc_ends = jnp.cumsum(doc_lengths)
    return jnp.sum((doc_ends[None, :] <= positions[:, None]).astype(jnp.int32), axis=1)


def pair_firsts(docs, pair_ids):
    doc_range = jnp.arange(pair_ids.shape[0], dtype=jnp.int32)
    own_pair = jnp.sum(jnp.where(docs[:, None] == doc_range[None, :], pair_ids[None, :], 0), axis=1)
    return jnp.sum((pair_ids[None, :] < own_pair[:, None]).astype(jnp.int32), axis=1)


def largest_divisor(total_rows, ceiling):
    return max(
        (
            candidate
            for candidate in range(1, min(total_rows, ceiling) + 1)
            if total_rows % candidate == 0
        )
    )


def attend(query_rows, positions, keys, values, doc_lengths, pair_ids):
    head_size = keys.shape[1]
    token_count = query_rows.shape[0]
    query_heads = query_rows.shape[1] // head_size
    shaped_queries = query_rows.reshape(token_count, query_heads, head_size)
    query_docs = token_docs(positions, doc_lengths)
    query_firsts = pair_firsts(query_docs, pair_ids)
    doc_range = jnp.arange(doc_lengths.shape[0], dtype=jnp.int32)
    pair_begin = jnp.sum(
        jnp.where(doc_range[None, :] < query_firsts[:, None], doc_lengths[None, :], 0), axis=1
    )
    lowest = jnp.min(pair_begin)
    highest = jnp.max(positions)
    scale = 1.0 / math.sqrt(head_size)

    def update(softmax_state, key_block, value_block, block_start):
        key_pos = block_start + jnp.arange(key_block.shape[0], dtype=jnp.int32)
        needed = (block_start <= highest) & (block_start + key_block.shape[0] > lowest)

        def compute(current):
            running_max, denominator, weighted = current
            key_docs = token_docs(key_pos, doc_lengths)
            allowed = (key_pos[None, :] <= positions[:, None]) & (
                (key_docs[None, :] == query_docs[:, None])
                | (key_docs[None, :] == query_firsts[:, None])
            )
            scores = (
                jnp.einsum(
                    "qhd,kd->hqk", shaped_queries, key_block, preferred_element_type=jnp.float32
                )
                * scale
            )
            newest = jnp.maximum(
                running_max, jnp.max(jnp.where(allowed[None], scores, NEGATIVE), axis=2)
            )
            weights = jnp.where(allowed[None], jnp.exp(scores - newest[:, :, None]), 0.0)
            factor = jnp.exp(running_max - newest)
            denominator = denominator * factor + jnp.sum(weights, axis=2)
            weighted = weighted * factor[:, :, None] + jnp.einsum(
                "hqk,kd->hqd",
                weights.astype(jnp.bfloat16),
                value_block,
                preferred_element_type=jnp.float32,
            )
            return (newest, denominator, weighted)

        def unchanged(current):
            return current

        return lax.cond(needed, compute, unchanged, softmax_state)

    initial = (
        jnp.full((query_heads, token_count), NEGATIVE, jnp.float32),
        jnp.zeros((query_heads, token_count), jnp.float32),
        jnp.zeros((query_heads, token_count, head_size), jnp.float32),
    )
    key_rows = lax.all_gather(keys, "seq", axis=0, tiled=True)
    value_rows = lax.all_gather(values, "seq", axis=0, tiled=True)
    row_total = key_rows.shape[0]
    block_rows = largest_divisor(row_total, 1024)
    block_count = row_total // block_rows
    stacked = (
        key_rows.reshape(block_count, block_rows, head_size),
        value_rows.reshape(block_count, block_rows, head_size),
        jnp.int32(0) + block_rows * jnp.arange(block_count, dtype=jnp.int32),
    )

    def advance(carried, block_item):
        return (update(carried, block_item[0], block_item[1], block_item[2]), None)

    result_state, unused_out = lax.scan(advance, initial, stacked)
    running_max, denominator, weighted = result_state
    attended = weighted / denominator[:, :, None]
    return (
        attended.transpose(1, 0, 2)
        .reshape(token_count, query_heads * head_size)
        .astype(jnp.bfloat16)
    )


def on_device(queries, keys, values, out_weight, doc_lengths, pair_ids, block_plan):
    seq_count = lax.axis_size("seq")
    my_seq = lax.axis_index("seq")
    shared_head = lax.axis_index("head") // 2
    key_rows = lax.dynamic_slice_in_dim(keys, shared_head * D_HEAD, D_HEAD, 1)
    value_rows = lax.dynamic_slice_in_dim(values, shared_head * D_HEAD, D_HEAD, 1)
    slots_here = seq_count // 2
    tok_rows = queries.shape[0]
    row_width = queries.shape[1]
    block_rows = tok_rows // slots_here
    slot_total = block_plan.shape[0]
    local_ids = my_seq * slots_here + jnp.arange(slots_here, dtype=jnp.int32)
    plan_rows = lax.dynamic_slice_in_dim(block_plan, my_seq * slots_here, slots_here, 0)
    planned_pos = (
        plan_rows[:, None] * block_rows + jnp.arange(block_rows, dtype=jnp.int32)[None, :]
    ).reshape(-1)
    slot_range = jnp.arange(slot_total, dtype=jnp.int32)
    target_slot = jnp.sum(
        jnp.where(block_plan[None, :] == local_ids[:, None], slot_range[None, :], 0), axis=1
    )
    device_range = jnp.arange(seq_count, dtype=jnp.int32)
    send_table = ((target_slot // slots_here)[:, None] == device_range[None, :]).astype(
        jnp.bfloat16
    )
    take_table = ((plan_rows // slots_here)[:, None] == device_range[None, :]).astype(jnp.bfloat16)
    blocked = queries.reshape(slots_here, block_rows, row_width)
    arrived = lax.all_to_all(
        jnp.einsum("bn,bkw->nkw", send_table, blocked, preferred_element_type=jnp.float32).astype(
            jnp.bfloat16
        ),
        "seq",
        split_axis=0,
        concat_axis=0,
        tiled=True,
    )
    chosen = jnp.einsum("bn,nkw->bkw", take_table, arrived, preferred_element_type=jnp.float32)
    attended = attend(
        chosen.astype(jnp.bfloat16).reshape(tok_rows, row_width),
        planned_pos,
        key_rows,
        value_rows,
        doc_lengths,
        pair_ids,
    )
    return lax.psum_scatter(
        jnp.dot(attended, out_weight, preferred_element_type=jnp.float32).astype(jnp.bfloat16),
        "head",
        scatter_dimension=0,
        tiled=True,
    )


FAR = 1e9
AHEAD = 3
EARLY = 2
ON = 6
PASS = 5


def direct(at):
    return (at < EARLY) | (lax.rem(at, 2) == 0)


def pick_tiles(width):
    return max(c for c in (1, 2, 4, 8, 16) if width % (c * 128) == 0)


def fused_kernel(
    seq_count,
    head_count,
    queries_hbm,
    keys_hbm,
    values_hbm,
    weight_hbm,
    pairs_ref,
    lens_ref,
    plan_ref,
    out_ref,
    queries_ref,
    keys_ref,
    values_ref,
    w_own,
    w_far,
    kv_all,
    q_send,
    q_recv_a,
    q_recv_b,
    q_heads,
    bias,
    attended,
    sent,
    arrived,
    final,
    load_sems,
    send_sems,
    kv_sems,
    q_sems,
    qz_sems,
    wz_sems,
    near_sems,
    rest_sems,
    a_sems,
    b_sems,
    f_sems,
):
    q_recv = (q_recv_a, q_recv_b)
    me = lax.axis_index("seq")
    rank = lax.axis_index("head")
    core = lax.rem(me, 2)
    partner = me + 1 - 2 * core
    along_x = me + 2 - 4 * lax.rem(me // 2, 2)
    along_y = lax.rem(me + seq_count // 2, seq_count)
    first = jnp.where(core == 0, along_x, along_y)
    second = jnp.where(core == 0, along_y, along_x)
    corner = along_x + along_y - me
    low = rank < head_count // 2
    inner = (rank > 0) & (rank < head_count - 1)
    mate = rank + 1 - 2 * lax.rem(rank, 2)
    across = head_count - 1 - rank
    slots, block_rows, width = queries_ref.shape
    tokens = slots * block_rows
    seq_len = seq_count * tokens
    pair_heads = width // (2 * D_HEAD)
    pair_width = pair_heads * D_HEAD
    shared = head_count // (keys_ref.shape[1] // D_HEAD)
    tiles, rows_all, tile = sent.shape
    half = tiles * tile
    share = width // (seq_count // 2)
    directs = sum(at < EARLY or at % 2 == 0 for at in range(tiles))

    def slot_at(place):
        at = (head_count - 1, head_count // 2, 0, 1)[place]
        return jnp.where(low, at, head_count - 1 - at)

    def share_rows(device):
        return pl.ds(pl.multiple_of((device // 2) * share, share), share)

    def tile_cols(at):
        return pl.ds(pl.multiple_of(at * tile, tile), tile)

    def out_cols(side, at):
        return pl.ds(pl.multiple_of(side * half + at * tile, tile), tile)

    own_copy = pltpu.make_async_copy(
        weight_hbm.at[:, pl.ds(pl.multiple_of(core * half, half), half)], w_own, load_sems.at[0]
    )

    queries_copy = pltpu.make_async_copy(queries_hbm, queries_ref, load_sems.at[1])
    kv_col = pl.ds(pl.multiple_of((rank // shared) * D_HEAD, D_HEAD), D_HEAD)
    mine = pl.ds(pl.multiple_of(me * tokens, tokens), tokens)
    keys_copy = pltpu.make_async_copy(keys_hbm, keys_ref, load_sems.at[2])
    values_copy = pltpu.make_async_copy(values_hbm, values_ref, load_sems.at[3])

    barrier = pltpu.get_barrier_semaphore()
    for step in range(1, seq_count):
        pl.semaphore_signal(barrier, inc=1, device_id={"seq": lax.rem(me + step, seq_count)})

    @pl.when(rank > 0)
    def _():
        pl.semaphore_signal(barrier, inc=1, device_id={"head": rank - 1})
        pl.semaphore_signal(barrier, inc=1, device_id={"seq": partner, "head": rank - 1})

    @pl.when(rank < head_count - 1)
    def _():
        pl.semaphore_signal(barrier, inc=1, device_id={"head": rank + 1})
        pl.semaphore_signal(barrier, inc=1, device_id={"seq": partner, "head": rank + 1})

    queries_copy.start()

    @pl.when(inner)
    def _():
        keys_copy.start()
        values_copy.start()
        own_copy.start()
        keys_copy.wait()
        values_copy.wait()
        kv_all[0, mine] = keys_ref[:, kv_col]
        kv_all[1, mine] = values_ref[:, kv_col]

    queries_copy.wait()
    for other in range(seq_count):
        local = jnp.int32(0)
        for slot in range(slots):
            offset = plan_ref[other * slots + slot] - me * slots
            local = local + jnp.where((offset >= 0) & (offset < slots), offset, 0)
        block = queries_ref[local]
        for part in range(2):
            q_send[part, other] = block[:, part * pair_width : (part + 1) * pair_width]
    for part in range(2):
        q_recv[part][me] = q_send[part, me]

    edges = jnp.where(rank > 0, 2, 0) + jnp.where(rank < head_count - 1, 2, 0)
    pl.semaphore_wait(barrier, seq_count - 1 + edges)

    def kv_copy(peer, slot, sem):
        rows = pl.ds(pl.multiple_of(slot * tokens, tokens), tokens)
        return pltpu.make_async_remote_copy(
            src_ref=kv_all.at[:, rows],
            dst_ref=kv_all.at[:, rows],
            send_sem=send_sems.at[0],
            recv_sem=kv_sems.at[sem],
            device_id={"seq": peer},
        )

    def q_copy(part, peer, slot):
        return pltpu.make_async_remote_copy(
            src_ref=q_send.at[part, peer],
            dst_ref=q_recv[part].at[slot],
            send_sem=send_sems.at[1],
            recv_sem=q_sems.at[part],
            device_id={"seq": peer},
        )

    def qz_copy(part, kept):
        return pltpu.make_async_remote_copy(
            src_ref=q_heads.at[0, part, kept],
            dst_ref=q_heads.at[1, part, kept],
            send_sem=send_sems.at[2],
            recv_sem=qz_sems.at[part, kept],
            device_id={"head": mate},
        )

    def wz_copy(at):
        return pltpu.make_async_remote_copy(
            src_ref=weight_hbm.at[share_rows(me), out_cols(core, at)],
            dst_ref=w_far.at[share_rows(me), tile_cols(at)],
            send_sem=send_sems.at[3],
            recv_sem=wz_sems.at[at],
            device_id={"head": mate},
        )

    def wd_copy(at):
        return pltpu.make_async_remote_copy(
            src_ref=weight_hbm.at[share_rows(corner), out_cols(core, at)],
            dst_ref=w_far.at[share_rows(corner), tile_cols(at)],
            send_sem=send_sems.at[4],
            recv_sem=rest_sems.at[at],
            device_id={"head": mate},
        )

    def relay(kind, source, peer, at):
        return pltpu.make_async_remote_copy(
            src_ref=w_far.at[share_rows(source), tile_cols(at)],
            dst_ref=w_far.at[share_rows(source), tile_cols(at)],
            send_sem=send_sems.at[5 + kind],
            recv_sem=(near_sems if kind == 0 else rest_sems).at[at],
            device_id={"seq": peer},
        )

    def a_copy(kept, side):
        return pltpu.make_async_remote_copy(
            src_ref=attended.at[kept, side],
            dst_ref=attended.at[kept, side],
            send_sem=send_sems.at[8],
            recv_sem=a_sems.at[kept],
            device_id={"seq": partner},
        )

    def side_rows(side):
        return pl.ds(pl.multiple_of(side * 2 * block_rows, block_rows), 2 * block_rows)

    def start_copy(side):
        return pltpu.make_async_remote_copy(
            src_ref=sent.at[0, side_rows(side)],
            dst_ref=arrived.at[0, side_rows(side)],
            send_sem=send_sems.at[9],
            recv_sem=b_sems.at[0],
            device_id={"head": across},
        )

    def b_copy(at):
        return pltpu.make_async_remote_copy(
            src_ref=sent.at[at],
            dst_ref=arrived.at[at],
            send_sem=send_sems.at[9],
            recv_sem=b_sems.at[at],
            device_id={"head": across},
        )

    def edge_copy(side, at, sender):
        return pltpu.make_async_remote_copy(
            src_ref=final.at[at, pl.ds(side * 2 * block_rows, block_rows)],
            dst_ref=out_ref.at[:, out_cols(sender, at)],
            send_sem=send_sems.at[10],
            recv_sem=f_sems.at[0],
            device_id={"seq": me - core + side, "head": mate},
        )

    def mate_copy(at, sender):
        rows = pl.ds(
            pl.multiple_of((3 - 2 * sender) * block_rows, block_rows), block_rows
        )
        return pltpu.make_async_remote_copy(
            src_ref=final.at[at, rows],
            dst_ref=out_ref.at[:, out_cols(sender, at)],
            send_sem=send_sems.at[10],
            recv_sem=f_sems.at[1],
            device_id={"seq": partner},
        )

    def out_copy(at):
        rows = pl.ds(
            pl.multiple_of((2 * core + 1) * block_rows, block_rows), block_rows
        )
        return pltpu.make_async_copy(
            final.at[at, rows], out_ref.at[:, out_cols(core, at)], send_sems.at[10]
        )

    def whole(ref, sem):
        pltpu.make_async_copy(ref, ref, sem).wait()

    @pl.when(inner)
    def _():
        for step in range(2, seq_count, 2):
            peer = lax.rem(me + step, seq_count)
            kv_copy(peer, me, step // 2 - 1).start()
        kv_copy(partner, me, 3).start()

    def push_corner(at):
        @pl.when(direct(at))
        def _():
            wd_copy(at).start()

    @pl.when(jnp.logical_not(inner))
    def _():
        for at in range(EARLY):
            wz_copy(at).start()
        push_corner(0)

    for part in range(2):
        for step in range(1, seq_count):
            peer = lax.rem(me + step, seq_count)
            q_copy(part, peer, me).start()

    def gather_queries(part):
        whole(q_recv[part].at[pl.ds(0, seq_count - 1)], q_sems.at[part])
        for place in range(slots):
            block = q_recv[part][plan_ref[me * slots + slot_at(place)] // slots]
            for head in range(pair_heads):
                row = ((place % 2) * pair_heads + head) * block_rows
                q_heads[0, part, place // 2, row : row + block_rows, :] = block[
                    :, head * D_HEAD : (head + 1) * D_HEAD
                ]

    @pl.when(jnp.logical_not(inner))
    def _():
        gather_queries(0)
        qz_copy(0, 0).start()
        wz_copy(2).start()
        gather_queries(1)
        qz_copy(1, 0).start()
        push_corner(1)
        wz_copy(3).start()
        push_corner(2)
        wz_copy(4).start()
        qz_copy(0, 1).start()
        qz_copy(1, 1).start()

        def push_next(at, carry):
            wz_copy(at).start()
            push_corner(at - 1)
            return carry

        lax.fori_loop(5, tiles, push_next, 0)
        push_corner(tiles - 1)
        whole(out_ref, f_sems.at[0])
        whole(weight_hbm.at[share_rows(me), pl.ds(0, half)], send_sems.at[3])
        whole(weight_hbm.at[share_rows(me), pl.ds(0, directs * tile)], send_sems.at[4])
        whole(q_heads.at[0], send_sems.at[2])

    @pl.when(inner)
    def _():
        row = lax.broadcasted_iota(jnp.int32, (tokens, 1), 0)
        position = row
        for place in range(slots):
            shift = (plan_ref[me * slots + slot_at(place)] - place) * block_rows
            here = (row >= place * block_rows) & (row < (place + 1) * block_rows)
            position = position + jnp.where(here, shift, 0)
        position = position.astype(jnp.float32)
        docs = pairs_ref.shape[1]
        doc_at = lax.broadcasted_iota(jnp.int32, (1, docs), 1)
        starts = jnp.zeros((1, docs), jnp.int32)
        ends = jnp.zeros((1, docs), jnp.int32)
        running = jnp.int32(0)
        for doc in range(docs):
            starts = jnp.where(doc_at == doc, running, starts)
            running = running + lens_ref[doc]
            ends = jnp.where(doc_at == doc, running, ends)
        starts = starts.astype(jnp.float32)
        ends = ends.astype(jnp.float32)
        pairs = pairs_ref[...].astype(jnp.float32)
        begun = starts <= position
        own_start = jnp.max(jnp.where(begun, starts, 0.0), axis=1, keepdims=True)
        own_pair = jnp.max(jnp.where(begun, pairs, 0.0), axis=1, keepdims=True)
        same = pairs == own_pair
        first_start = jnp.min(jnp.where(same, starts, FAR), axis=1, keepdims=True)
        first_end = jnp.min(jnp.where(same, ends, FAR), axis=1, keepdims=True)
        key_width = 2 * D_HEAD
        parts = seq_len // key_width
        for part in range(parts):
            key_pos = (
                lax.broadcasted_iota(jnp.int32, (tokens, key_width), 1) + part * key_width
            ).astype(jnp.float32)
            seen = (key_pos <= position) & (
                (key_pos >= own_start) | ((key_pos >= first_start) & (key_pos < first_end))
            )
            bias[part] = jnp.where(seen, 0.0, NEGATIVE)

        for step in range(2, seq_count, 2):
            source = lax.rem(me + seq_count - step, seq_count)
            kv_copy(partner, source, step // 2 - 1).wait_recv()
            kv_copy(partner, source, 3).start()

        def pass_on(at):
            wz_copy(at).wait_recv()
            relay(0, me, first, at).start()
            relay(1, me, second, at).start()

        def pass_far(at):
            @pl.when(jnp.logical_not(direct(at)))
            def _():
                relay(0, first, first, at).wait_recv()
                relay(2, first, second, at).start()

        def complete(at):
            @pl.when(direct(at))
            def _():
                relay(0, first, first, at).wait_recv()

            whole(w_far.at[pl.ds(0, 2 * share), tile_cols(at)], rest_sems.at[at])

        pass_on(0)
        gather_queries(0)
        pass_on(1)
        whole(kv_all.at[:, pl.ds(0, seq_count // 2 * tokens)], kv_sems.at[3])

        scale = math.log2(math.e) / math.sqrt(D_HEAD)

        def unit(group, part, kept):
            rows_q = q_heads[group, part, kept]
            scores = []
            for block in range(parts):
                masks = []
                for kind in range(2):
                    rows_at = (2 * kept + kind) * block_rows
                    masks += [bias[block, rows_at : rows_at + block_rows, :]] * pair_heads
                scores.append(
                    lax.dot_general(
                        rows_q,
                        kv_all[0, block * key_width : (block + 1) * key_width],
                        (((1,), (1,)), ((), ())),
                        preferred_element_type=jnp.float32,
                    )
                    * scale
                    + jnp.concatenate(masks, axis=0)
                )
            top = functools.reduce(jnp.maximum, scores)
            top = jnp.max(top, axis=1, keepdims=True)
            total = jnp.zeros((2 * pair_heads * block_rows, key_width), jnp.float32)
            summed = jnp.zeros((2 * pair_heads * block_rows, D_HEAD), jnp.float32)
            for block in range(parts):
                weights = jnp.exp2(scores[block] - top)
                total = total + weights
                summed = summed + jnp.dot(
                    weights.astype(jnp.bfloat16),
                    kv_all[1, block * key_width : (block + 1) * key_width],
                    preferred_element_type=jnp.float32,
                )
            total = jnp.sum(total, axis=1, keepdims=True)
            result = (summed / total).astype(jnp.bfloat16)
            for kind in range(2):
                for head in range(pair_heads):
                    row = (kind * pair_heads + head) * block_rows
                    at = ((group * 2 + part) * pair_heads + head) * D_HEAD
                    attended[kept, core, kind, :, pl.ds(pl.multiple_of(at, D_HEAD), D_HEAD)] = (
                        result[row : row + block_rows]
                    )

        def product(rows_a, at):
            return jnp.dot(
                rows_a[:, :width], w_own[:, tile_cols(at)], preferred_element_type=jnp.float32
            ) + jnp.dot(
                rows_a[:, width:], w_far[:, tile_cols(at)], preferred_element_type=jnp.float32
            )

        def half_term(side):
            rows_a = attended[0, side].reshape(2 * block_rows, 2 * width)
            sent[0, side_rows(side)] = product(rows_a, 0).astype(jnp.bfloat16)
            start_copy(side).start()

        def term(kept, at):
            return product(attended[kept].reshape(rows_all, 2 * width), at)

        def send_term(at):
            complete(at)
            sent[at] = term(0, at).astype(jnp.bfloat16)
            b_copy(at).start()

        def keep_term(at):
            mixed = term(1, at)

            b_copy(at).wait_recv()
            final[at] = (mixed + arrived[at].astype(jnp.float32)).astype(jnp.bfloat16)
            edge_copy(0, at, core).start()
            edge_copy(1, at, core).start()
            mate_copy(at, core).start()
            out_copy(at).start()

        def sent_unit(item, carry):
            @pl.when(item == 1)
            def _():
                gather_queries(1)

            @pl.when(item >= 2)
            def _():
                qz_copy(item - 2, 0).wait_recv()

            unit(item // 2, lax.rem(item, 2), 0)
            return carry

        def kept_unit(item, carry):
            @pl.when(item >= 2)
            def _():
                qz_copy(item - 2, 1).wait_recv()

            unit(item // 2, lax.rem(item, 2), 1)
            return carry

        lax.fori_loop(0, 4, sent_unit, 0)
        a_copy(0, core).start()
        own_copy.wait()
        complete(0)
        half_term(core)
        pass_on(2)
        a_copy(0, 1 - core).wait_recv()
        half_term(1 - core)
        send_term(1)
        pass_on(3)
        lax.fori_loop(0, 2, kept_unit, 0)
        pass_on(4)
        send_term(2)
        pass_far(3)
        lax.fori_loop(2, 4, kept_unit, 0)
        a_copy(1, core).start()
        for at in range(5, ON):
            pass_on(at)
        for at in range(3, AHEAD):
            send_term(at)
        for at in range(4, PASS):
            pass_far(at)
        a_copy(1, 1 - core).wait_recv()

        def advance(at, carry):
            @pl.when(at + PASS < tiles)
            def _():
                pass_far(at + PASS)

            @pl.when(at + ON < tiles)
            def _():
                pass_on(at + ON)

            @pl.when(at + AHEAD < tiles)
            def _():
                send_term(at + AHEAD)

            keep_term(at)
            return carry

        lax.fori_loop(0, tiles, advance, 0)

        whole(final, send_sems.at[10])
        whole(sent, send_sems.at[9])
        whole(attended.at[0], send_sems.at[8])
        whole(w_far.at[pl.ds(0, share)], send_sems.at[5])
        whole(w_far.at[pl.ds(0, share)], send_sems.at[6])
        whole(w_far.at[pl.ds(0, share), pl.ds(0, (tiles - directs) * tile)], send_sems.at[7])
        whole(kv_all.at[:, pl.ds(0, (seq_count - 1) * tokens)], send_sems.at[0])
        whole(out_ref.at[:, pl.ds(0, half)], f_sems.at[1])

    whole(q_send.at[:, pl.ds(0, seq_count - 1)], send_sems.at[1])


def fused_device(queries, keys, values, out_weight, doc_lengths, pair_ids, block_plan):
    seq_count = lax.axis_size("seq")
    head_count = lax.axis_size("head")
    tokens, width = queries.shape
    slots = block_plan.shape[0] // seq_count
    block_rows = tokens // slots
    out_width = out_weight.shape[1]
    half_width = out_width // 2
    tiles = pick_tiles(half_width)
    tile = half_width // tiles
    half = jnp.bfloat16
    flow = pltpu.VMEM((tiles, 4 * block_rows, tile), half)
    weights = pltpu.VMEM((width, half_width), half)
    in_vmem = pl.BlockSpec(memory_space=pltpu.VMEM)
    anywhere = pl.BlockSpec(memory_space=pl.ANY)
    in_smem = pl.BlockSpec(memory_space=pltpu.SMEM)
    dma = pltpu.SemaphoreType.DMA
    return pl.pallas_call(
        functools.partial(fused_kernel, seq_count, head_count),
        out_shape=jax.ShapeDtypeStruct((block_rows, out_width), half),
        in_specs=[anywhere, anywhere, anywhere, anywhere, in_vmem, in_smem, in_smem],
        out_specs=anywhere,
        scratch_shapes=[
            pltpu.VMEM((slots, block_rows, width), half),
            pltpu.VMEM(keys.shape, half),
            pltpu.VMEM(values.shape, half),
            weights,
            weights,
            pltpu.VMEM((2, seq_count * tokens, D_HEAD), half),
            pltpu.VMEM((2, seq_count, block_rows, width // 2), half),
            pltpu.VMEM((seq_count, block_rows, width // 2), half),
            pltpu.VMEM((seq_count, block_rows, width // 2), half),
            pltpu.VMEM((2, 2, 2, width // D_HEAD * block_rows, D_HEAD), half),
            pltpu.VMEM(
                (seq_count * tokens // (2 * D_HEAD), tokens, 2 * D_HEAD), jnp.float32
            ),
            pltpu.VMEM((2, 2, 2, block_rows, 2 * width), half),
            flow,
            flow,
            flow,
            dma((4,)),
            dma((11,)),
            dma((4,)),
            dma((2,)),
            dma((2, 2)),
            dma((tiles,)),
            dma((tiles,)),
            dma((tiles,)),
            dma((2,)),
            dma((tiles,)),
            dma((2,)),
        ],
        compiler_params=pltpu.CompilerParams(
            collective_id=0, has_side_effects=True, vmem_limit_bytes=60000 * 1024
        ),
    )(
        queries.reshape(slots, block_rows, width),
        keys,
        values,
        out_weight,
        pair_ids[None],
        doc_lengths,
        block_plan,
    )


def pick_device(queries, keys, values, out_weight, doc_lengths, pair_ids, block_plan):
    seq_count = lax.axis_size("seq")
    head_count = lax.axis_size("head")
    tokens, width = queries.shape
    out_width = out_weight.shape[1]
    block_rows = tokens * seq_count // block_plan.shape[0]
    fits = seq_count * tokens * tokens * 4 <= 4 * 1024 * 1024
    shape = head_count == 4 and seq_count == 8 and keys.shape[1] == 2 * D_HEAD and width % (2 * D_HEAD) == 0
    square = block_rows * head_count == tokens and block_rows % 16 == 0
    even = seq_count * tokens % (2 * D_HEAD) == 0 and width % 64 == 0
    wide = out_width % 2 == 0 and out_width // 2 % (16 * 128) == 0
    run = fused_device if fits and shape and square and even and wide else on_device
    return run(queries, keys, values, out_weight, doc_lengths, pair_ids, block_plan)


def solution(mesh):
    return jax.shard_map(
        pick_device,
        mesh=mesh,
        in_specs=(P("seq", "head"), P("seq", None), P("seq", None), P("head", None), P(), P(), P()),
        out_specs=P(("seq", "head"), None),
        check_vma=False,
    )
```

```python
import functools
import math

import jax
import jax.numpy as jnp
from jax import lax
from jax.experimental import pallas as pl
from jax.experimental.pallas import tpu as pltpu
from jax.sharding import PartitionSpec as P

D_HEAD = 128


NEGATIVE = -1e30


def token_docs(positions, doc_lengths):
    doc_ends = jnp.cumsum(doc_lengths)
    return jnp.sum((doc_ends[None, :] <= positions[:, None]).astype(jnp.int32), axis=1)


def pair_firsts(docs, pair_ids):
    doc_range = jnp.arange(pair_ids.shape[0], dtype=jnp.int32)
    own_pair = jnp.sum(jnp.where(docs[:, None] == doc_range[None, :], pair_ids[None, :], 0), axis=1)
    return jnp.sum((pair_ids[None, :] < own_pair[:, None]).astype(jnp.int32), axis=1)


def largest_divisor(total_rows, ceiling):
    return max(
        (
            candidate
            for candidate in range(1, min(total_rows, ceiling) + 1)
            if total_rows % candidate == 0
        )
    )


def attend(query_rows, positions, keys, values, doc_lengths, pair_ids):
    head_size = keys.shape[1]
    token_count = query_rows.shape[0]
    query_heads = query_rows.shape[1] // head_size
    shaped_queries = query_rows.reshape(token_count, query_heads, head_size)
    query_docs = token_docs(positions, doc_lengths)
    query_firsts = pair_firsts(query_docs, pair_ids)
    doc_range = jnp.arange(doc_lengths.shape[0], dtype=jnp.int32)
    pair_begin = jnp.sum(
        jnp.where(doc_range[None, :] < query_firsts[:, None], doc_lengths[None, :], 0), axis=1
    )
    lowest = jnp.min(pair_begin)
    highest = jnp.max(positions)
    scale = 1.0 / math.sqrt(head_size)

    def update(softmax_state, key_block, value_block, block_start):
        key_pos = block_start + jnp.arange(key_block.shape[0], dtype=jnp.int32)
        needed = (block_start <= highest) & (block_start + key_block.shape[0] > lowest)

        def compute(current):
            running_max, denominator, weighted = current
            key_docs = token_docs(key_pos, doc_lengths)
            allowed = (key_pos[None, :] <= positions[:, None]) & (
                (key_docs[None, :] == query_docs[:, None])
                | (key_docs[None, :] == query_firsts[:, None])
            )
            scores = (
                jnp.einsum(
                    "qhd,kd->hqk", shaped_queries, key_block, preferred_element_type=jnp.float32
                )
                * scale
            )
            newest = jnp.maximum(
                running_max, jnp.max(jnp.where(allowed[None], scores, NEGATIVE), axis=2)
            )
            weights = jnp.where(allowed[None], jnp.exp(scores - newest[:, :, None]), 0.0)
            factor = jnp.exp(running_max - newest)
            denominator = denominator * factor + jnp.sum(weights, axis=2)
            weighted = weighted * factor[:, :, None] + jnp.einsum(
                "hqk,kd->hqd",
                weights.astype(jnp.bfloat16),
                value_block,
                preferred_element_type=jnp.float32,
            )
            return (newest, denominator, weighted)

        def unchanged(current):
            return current

        return lax.cond(needed, compute, unchanged, softmax_state)

    initial = (
        jnp.full((query_heads, token_count), NEGATIVE, jnp.float32),
        jnp.zeros((query_heads, token_count), jnp.float32),
        jnp.zeros((query_heads, token_count, head_size), jnp.float32),
    )
    key_rows = lax.all_gather(keys, "seq", axis=0, tiled=True)
    value_rows = lax.all_gather(values, "seq", axis=0, tiled=True)
    row_total = key_rows.shape[0]
    block_rows = largest_divisor(row_total, 1024)
    block_count = row_total // block_rows
    stacked = (
        key_rows.reshape(block_count, block_rows, head_size),
        value_rows.reshape(block_count, block_rows, head_size),
        jnp.int32(0) + block_rows * jnp.arange(block_count, dtype=jnp.int32),
    )

    def advance(carried, block_item):
        return (update(carried, block_item[0], block_item[1], block_item[2]), None)

    result_state, unused_out = lax.scan(advance, initial, stacked)
    running_max, denominator, weighted = result_state
    attended = weighted / denominator[:, :, None]
    return (
        attended.transpose(1, 0, 2)
        .reshape(token_count, query_heads * head_size)
        .astype(jnp.bfloat16)
    )


def on_device(queries, keys, values, out_weight, doc_lengths, pair_ids, block_plan):
    seq_count = lax.axis_size("seq")
    my_seq = lax.axis_index("seq")
    shared_head = lax.axis_index("head") // 2
    key_rows = lax.dynamic_slice_in_dim(keys, shared_head * D_HEAD, D_HEAD, 1)
    value_rows = lax.dynamic_slice_in_dim(values, shared_head * D_HEAD, D_HEAD, 1)
    slots_here = seq_count // 2
    tok_rows = queries.shape[0]
    row_width = queries.shape[1]
    block_rows = tok_rows // slots_here
    slot_total = block_plan.shape[0]
    local_ids = my_seq * slots_here + jnp.arange(slots_here, dtype=jnp.int32)
    plan_rows = lax.dynamic_slice_in_dim(block_plan, my_seq * slots_here, slots_here, 0)
    planned_pos = (
        plan_rows[:, None] * block_rows + jnp.arange(block_rows, dtype=jnp.int32)[None, :]
    ).reshape(-1)
    slot_range = jnp.arange(slot_total, dtype=jnp.int32)
    target_slot = jnp.sum(
        jnp.where(block_plan[None, :] == local_ids[:, None], slot_range[None, :], 0), axis=1
    )
    device_range = jnp.arange(seq_count, dtype=jnp.int32)
    send_table = ((target_slot // slots_here)[:, None] == device_range[None, :]).astype(
        jnp.bfloat16
    )
    take_table = ((plan_rows // slots_here)[:, None] == device_range[None, :]).astype(jnp.bfloat16)
    blocked = queries.reshape(slots_here, block_rows, row_width)
    arrived = lax.all_to_all(
        jnp.einsum("bn,bkw->nkw", send_table, blocked, preferred_element_type=jnp.float32).astype(
            jnp.bfloat16
        ),
        "seq",
        split_axis=0,
        concat_axis=0,
        tiled=True,
    )
    chosen = jnp.einsum("bn,nkw->bkw", take_table, arrived, preferred_element_type=jnp.float32)
    attended = attend(
        chosen.astype(jnp.bfloat16).reshape(tok_rows, row_width),
        planned_pos,
        key_rows,
        value_rows,
        doc_lengths,
        pair_ids,
    )
    return lax.psum_scatter(
        jnp.dot(attended, out_weight, preferred_element_type=jnp.float32).astype(jnp.bfloat16),
        "head",
        scatter_dimension=0,
        tiled=True,
    )


FAR = 1e9
AHEAD = 5
EARLY = 4
ON = 11


def pick_tiles(width):
    return max(c for c in (1, 2, 4, 8) if width % (c * 128) == 0)


def fused_kernel(
    seq_count,
    head_count,
    queries_hbm,
    keys_hbm,
    values_hbm,
    weight_hbm,
    pairs_ref,
    lens_ref,
    plan_ref,
    out_ref,
    queries_ref,
    keys_ref,
    values_ref,
    w_own,
    w_far,
    kv_all,
    q_send,
    q_recv_a,
    q_recv_b,
    q_heads,
    bias,
    attended,
    sent,
    arrived,
    final,
    load_sems,
    send_sems,
    kv_sems,
    q_sems,
    qz_sems,
    wz_sems,
    near_sems,
    a_sems,
    b_sems,
    f_sems,
):
    q_recv = (q_recv_a, q_recv_b)
    me = lax.axis_index("seq")
    rank = lax.axis_index("head")
    core = lax.rem(me, 2)
    partner = me + 1 - 2 * core
    along_x = me + 2 - 4 * lax.rem(me // 2, 2)
    along_y = lax.rem(me + seq_count // 2, seq_count)
    quad = lax.rem(me, 4)
    base = me - quad
    side = quad // 2
    low = rank < head_count // 2
    inner = (rank > 0) & (rank < head_count - 1)
    mate = rank + 1 - 2 * lax.rem(rank, 2)
    across = head_count - 1 - rank
    slots, block_rows, width = queries_ref.shape
    tokens = slots * block_rows
    seq_len = seq_count * tokens
    pair_heads = width // (2 * D_HEAD)
    pair_width = pair_heads * D_HEAD
    shared = head_count // (keys_ref.shape[1] // D_HEAD)
    messages, rows_all, tile = sent.shape
    tiles = messages // 2
    quarter = tiles * tile
    share = width // (seq_count // 4)
    piece = share // 2

    def slot_at(place):
        at = (head_count - 1, head_count // 2, 0, 1)[place]
        return jnp.where(low, at, head_count - 1 - at)

    def piece_rows(device, at):
        return pl.ds(
            pl.multiple_of((device // 4) * share + lax.rem(at, 2) * piece, piece), piece
        )

    def tile_cols(at):
        return pl.ds(pl.multiple_of(at * tile, tile), tile)

    def out_cols(owner, at):
        return pl.ds(pl.multiple_of(owner * quarter + at * tile, tile), tile)

    def order(message):
        message = jnp.int32(message)
        last = message >= messages - 2
        odd = lax.rem(message, 2) == 1
        other = last | ((message >= 3) & odd)
        at = jnp.where(odd, (message - 3) // 2, (message + 2) // 2)
        at = jnp.where(last, message - tiles, jnp.where(message < 3, message, at))
        return at, other

    own_copy = pltpu.make_async_copy(
        weight_hbm.at[:, pl.ds(pl.multiple_of(quad * quarter, quarter), quarter)],
        w_own,
        load_sems.at[0],
    )
    queries_copy = pltpu.make_async_copy(queries_hbm, queries_ref, load_sems.at[1])
    kv_col = pl.ds(pl.multiple_of((rank // shared) * D_HEAD, D_HEAD), D_HEAD)
    mine = pl.ds(pl.multiple_of(me * tokens, tokens), tokens)
    keys_copy = pltpu.make_async_copy(keys_hbm, keys_ref, load_sems.at[2])
    values_copy = pltpu.make_async_copy(values_hbm, values_ref, load_sems.at[3])

    barrier = pltpu.get_barrier_semaphore()
    for step in range(1, seq_count):
        pl.semaphore_signal(barrier, inc=1, device_id={"seq": lax.rem(me + step, seq_count)})

    for place in range(4):
        pl.semaphore_signal(barrier, inc=1, device_id={"seq": base + place, "head": mate})

    @pl.when(inner)
    def _():
        pl.semaphore_signal(barrier, inc=1, device_id={"head": across})

    queries_copy.start()

    @pl.when(inner)
    def _():
        keys_copy.start()
        values_copy.start()
        own_copy.start()
        keys_copy.wait()
        values_copy.wait()
        kv_all[0, mine] = keys_ref[:, kv_col]
        kv_all[1, mine] = values_ref[:, kv_col]

    queries_copy.wait()
    for other in range(seq_count):
        local = jnp.int32(0)
        for slot in range(slots):
            offset = plan_ref[other * slots + slot] - me * slots
            local = local + jnp.where((offset >= 0) & (offset < slots), offset, 0)
        block = queries_ref[local]
        for part in range(2):
            q_send[part, other] = block[:, part * pair_width : (part + 1) * pair_width]
    for part in range(2):
        q_recv[part][me] = q_send[part, me]

    pl.semaphore_wait(barrier, seq_count + 3 + jnp.where(inner, 1, 0))

    def kv_copy(peer, slot, sem):
        rows = pl.ds(pl.multiple_of(slot * tokens, tokens), tokens)
        return pltpu.make_async_remote_copy(
            src_ref=kv_all.at[:, rows],
            dst_ref=kv_all.at[:, rows],
            send_sem=send_sems.at[0],
            recv_sem=kv_sems.at[sem],
            device_id={"seq": peer},
        )

    def q_copy(part, peer, slot):
        return pltpu.make_async_remote_copy(
            src_ref=q_send.at[part, peer],
            dst_ref=q_recv[part].at[slot],
            send_sem=send_sems.at[1],
            recv_sem=q_sems.at[part],
            device_id={"seq": peer},
        )

    def qz_copy(part, kept):
        return pltpu.make_async_remote_copy(
            src_ref=q_heads.at[0, part, kept],
            dst_ref=q_heads.at[1, part, kept],
            send_sem=send_sems.at[2],
            recv_sem=qz_sems.at[part, kept],
            device_id={"head": mate},
        )

    def wz_copy(at):
        rows = piece_rows(me, at)
        return pltpu.make_async_remote_copy(
            src_ref=weight_hbm.at[rows, out_cols(quad, at // 2)],
            dst_ref=w_far.at[rows, tile_cols(at // 2)],
            send_sem=send_sems.at[3],
            recv_sem=wz_sems.at[at],
            device_id={"head": mate},
        )

    def relay(at):
        rows = piece_rows(me, at)
        return pltpu.make_async_remote_copy(
            src_ref=w_far.at[rows, tile_cols(at // 2)],
            dst_ref=w_far.at[rows, tile_cols(at // 2)],
            send_sem=send_sems.at[5],
            recv_sem=near_sems.at[at // 2],
            device_id={"seq": along_y},
        )

    def a_copy(kept, group, kind, peer):
        cols = pl.ds(group * width, width)
        return pltpu.make_async_remote_copy(
            src_ref=attended.at[kept, side, core, :, :, cols],
            dst_ref=attended.at[kept, side, core, :, :, cols],
            send_sem=send_sems.at[8],
            recv_sem=a_sems.at[kept, kind],
            device_id={"seq": peer},
        )

    def far_copy(kept):
        return pltpu.make_async_remote_copy(
            src_ref=attended.at[kept, 1 - side, core],
            dst_ref=attended.at[kept, 1 - side, core],
            send_sem=send_sems.at[7],
            recv_sem=a_sems.at[kept, 2],
            device_id={"seq": partner},
        )

    def core_rows(which):
        return pl.ds(pl.multiple_of(which * 2 * block_rows, block_rows), 2 * block_rows)

    def start_copy(which):
        return pltpu.make_async_remote_copy(
            src_ref=sent.at[0, core_rows(which)],
            dst_ref=arrived.at[0, core_rows(which)],
            send_sem=send_sems.at[9],
            recv_sem=b_sems.at[0],
            device_id={"head": across},
        )

    def b_copy(at):
        return pltpu.make_async_remote_copy(
            src_ref=sent.at[at],
            dst_ref=arrived.at[at],
            send_sem=send_sems.at[9],
            recv_sem=b_sems.at[at],
            device_id={"head": across},
        )

    def kind_rows(which, kind):
        return pl.ds(pl.multiple_of((2 * which + kind) * block_rows, block_rows), block_rows)

    def edge_copy(message, at, half, which):
        return pltpu.make_async_remote_copy(
            src_ref=final.at[message, kind_rows(which, 0)],
            dst_ref=out_ref.at[:, out_cols(quad, at)],
            send_sem=send_sems.at[10],
            recv_sem=f_sems.at[0],
            device_id={"seq": base + 2 * half + which, "head": mate},
        )

    def inner_copy(message, at, half, which):
        return pltpu.make_async_remote_copy(
            src_ref=final.at[message, kind_rows(which, 1)],
            dst_ref=out_ref.at[:, out_cols(quad, at)],
            send_sem=send_sems.at[10],
            recv_sem=f_sems.at[1],
            device_id={"seq": base + 2 * half + which},
        )

    def out_copy(message, at):
        return pltpu.make_async_copy(
            final.at[message, kind_rows(core, 1)],
            out_ref.at[:, out_cols(quad, at)],
            send_sems.at[10],
        )

    def whole(ref, sem):
        pltpu.make_async_copy(ref, ref, sem).wait()

    @pl.when(inner)
    def _():
        for step in range(2, seq_count, 2):
            peer = lax.rem(me + step, seq_count)
            kv_copy(peer, me, step // 2 - 1).start()
        kv_copy(partner, me, 3).start()

    @pl.when(jnp.logical_not(inner))
    def _():
        for at in range(EARLY):
            wz_copy(at).start()

    for part in range(2):
        for step in range(1, seq_count):
            peer = lax.rem(me + step, seq_count)
            q_copy(part, peer, me).start()

    def gather_queries(part):
        whole(q_recv[part].at[pl.ds(0, seq_count - 1)], q_sems.at[part])
        for place in range(slots):
            block = q_recv[part][plan_ref[me * slots + slot_at(place)] // slots]
            for head in range(pair_heads):
                row = ((place % 2) * pair_heads + head) * block_rows
                q_heads[0, part, place // 2, row : row + block_rows, :] = block[
                    :, head * D_HEAD : (head + 1) * D_HEAD
                ]

    @pl.when(jnp.logical_not(inner))
    def _():
        gather_queries(0)
        qz_copy(0, 0).start()
        gather_queries(1)
        qz_copy(1, 0).start()
        for at in range(EARLY, EARLY + 4):
            wz_copy(at).start()
        qz_copy(0, 1).start()
        qz_copy(1, 1).start()

        def push_next(at, carry):
            wz_copy(at).start()
            return carry

        lax.fori_loop(EARLY + 4, messages, push_next, 0)
        whole(out_ref, f_sems.at[0])
        whole(weight_hbm.at[pl.ds(0, share), pl.ds(0, quarter)], send_sems.at[3])
        whole(q_heads.at[0], send_sems.at[2])

    @pl.when(inner)
    def _():
        row = lax.broadcasted_iota(jnp.int32, (tokens, 1), 0)
        position = row
        for place in range(slots):
            shift = (plan_ref[me * slots + slot_at(place)] - place) * block_rows
            here = (row >= place * block_rows) & (row < (place + 1) * block_rows)
            position = position + jnp.where(here, shift, 0)
        position = position.astype(jnp.float32)
        docs = pairs_ref.shape[1]
        doc_at = lax.broadcasted_iota(jnp.int32, (1, docs), 1)
        starts = jnp.zeros((1, docs), jnp.int32)
        ends = jnp.zeros((1, docs), jnp.int32)
        running = jnp.int32(0)
        for doc in range(docs):
            starts = jnp.where(doc_at == doc, running, starts)
            running = running + lens_ref[doc]
            ends = jnp.where(doc_at == doc, running, ends)
        starts = starts.astype(jnp.float32)
        ends = ends.astype(jnp.float32)
        pairs = pairs_ref[...].astype(jnp.float32)
        begun = starts <= position
        own_start = jnp.max(jnp.where(begun, starts, 0.0), axis=1, keepdims=True)
        own_pair = jnp.max(jnp.where(begun, pairs, 0.0), axis=1, keepdims=True)
        same = pairs == own_pair
        first_start = jnp.min(jnp.where(same, starts, FAR), axis=1, keepdims=True)
        first_end = jnp.min(jnp.where(same, ends, FAR), axis=1, keepdims=True)
        key_width = 2 * D_HEAD
        parts = seq_len // key_width
        for part in range(parts):
            key_pos = (
                lax.broadcasted_iota(jnp.int32, (tokens, key_width), 1) + part * key_width
            ).astype(jnp.float32)
            seen = (key_pos <= position) & (
                (key_pos >= own_start) | ((key_pos >= first_start) & (key_pos < first_end))
            )
            bias[part] = jnp.where(seen, 0.0, NEGATIVE)

        for step in range(2, seq_count, 2):
            source = lax.rem(me + seq_count - step, seq_count)
            kv_copy(partner, source, step // 2 - 1).wait_recv()
            kv_copy(partner, source, 3).start()

        def pass_on(at):
            wz_copy(at).wait_recv()
            relay(at).start()

        def complete(at):
            whole(w_far.at[pl.ds(0, share), tile_cols(at)], near_sems.at[at])

        pass_on(0)
        pass_on(1)
        gather_queries(0)
        pass_on(2)
        whole(kv_all.at[:, pl.ds(0, seq_count // 2 * tokens)], kv_sems.at[3])

        scale = math.log2(math.e) / math.sqrt(D_HEAD)

        def unit(group, part, kept):
            rows_q = q_heads[group, part, kept]
            scores = []
            for block in range(parts):
                masks = []
                for kind in range(2):
                    rows_at = (2 * kept + kind) * block_rows
                    masks += [bias[block, rows_at : rows_at + block_rows, :]] * pair_heads
                scores.append(
                    lax.dot_general(
                        rows_q,
                        kv_all[0, block * key_width : (block + 1) * key_width],
                        (((1,), (1,)), ((), ())),
                        preferred_element_type=jnp.float32,
                    )
                    * scale
                    + jnp.concatenate(masks, axis=0)
                )
            top = functools.reduce(jnp.maximum, scores)
            top = jnp.max(top, axis=1, keepdims=True)
            total = jnp.zeros((2 * pair_heads * block_rows, key_width), jnp.float32)
            summed = jnp.zeros((2 * pair_heads * block_rows, D_HEAD), jnp.float32)
            for block in range(parts):
                weights = jnp.exp2(scores[block] - top)
                total = total + weights
                summed = summed + jnp.dot(
                    weights.astype(jnp.bfloat16),
                    kv_all[1, block * key_width : (block + 1) * key_width],
                    preferred_element_type=jnp.float32,
                )
            total = jnp.sum(total, axis=1, keepdims=True)
            result = (summed / total).astype(jnp.bfloat16)
            for kind in range(2):
                for head in range(pair_heads):
                    row = (kind * pair_heads + head) * block_rows
                    at = ((group * 2 + part) * pair_heads + head) * D_HEAD
                    attended[kept, side, core, kind, :, pl.ds(pl.multiple_of(at, D_HEAD), D_HEAD)] = (
                        result[row : row + block_rows]
                    )

        def product(rows_a, at):
            return jnp.dot(
                rows_a[:, :width], w_own[:, tile_cols(at)], preferred_element_type=jnp.float32
            ) + jnp.dot(
                rows_a[:, width:], w_far[:, tile_cols(at)], preferred_element_type=jnp.float32
            )

        def half_term(which):
            rows_a = attended[0, side, which].reshape(2 * block_rows, 2 * width)
            sent[0, core_rows(which)] = product(rows_a, 0).astype(jnp.bfloat16)
            start_copy(which).start()

        def term(kept, half, at):
            return product(attended[kept, half].reshape(rows_all, 2 * width), at)

        def send_term(message):
            at, other = order(message)

            @pl.when(jnp.logical_not(other))
            def _():
                complete(at)

            half = jnp.where(other, 1 - side, side)
            sent[message] = term(0, half, at).astype(jnp.bfloat16)
            b_copy(message).start()

        def keep_term(message):
            at, other = order(message)
            half = jnp.where(other, 1 - side, side)
            mixed = term(1, half, at)
            b_copy(message).wait_recv()
            final[message] = (mixed + arrived[message].astype(jnp.float32)).astype(jnp.bfloat16)
            edge_copy(message, at, half, 0).start()
            edge_copy(message, at, half, 1).start()
            inner_copy(message, at, half, 1 - core).start()

            @pl.when(other)
            def _():
                inner_copy(message, at, half, core).start()

            @pl.when(jnp.logical_not(other))
            def _():
                out_copy(message, at).start()

        def share_out(kept, group):
            a_copy(kept, group, 1, along_x).start()
            a_copy(kept, group, 0, partner).start()

        def wait_rows(kept, kind):
            whole(attended.at[kept, 0, 0], a_sems.at[kept, kind])

        def sent_unit(item, carry):
            @pl.when(item == 1)
            def _():
                gather_queries(1)
                pass_on(3)

            @pl.when(item >= 2)
            def _():
                qz_copy(item - 2, 0).wait_recv()

            unit(item // 2, lax.rem(item, 2), 0)

            @pl.when(item == 1)
            def _():
                share_out(0, 0)

            return carry

        def kept_unit(item, carry):
            @pl.when(item >= 2)
            def _():
                qz_copy(item - 2, 1).wait_recv()

            unit(item // 2, lax.rem(item, 2), 1)
            return carry

        lax.fori_loop(0, 4, sent_unit, 0)
        share_out(0, 1)
        own_copy.wait()
        pass_on(4)
        complete(0)
        half_term(core)
        wait_rows(0, 0)
        half_term(1 - core)
        pass_on(5)
        send_term(1)
        lax.fori_loop(0, 2, kept_unit, 0)
        share_out(1, 0)
        pass_on(6)
        send_term(2)
        wait_rows(0, 1)
        far_copy(0).start()
        pass_on(7)
        wait_rows(0, 2)
        send_term(3)
        pass_on(8)
        lax.fori_loop(2, 4, kept_unit, 0)
        share_out(1, 1)
        pass_on(9)
        send_term(4)
        pass_on(10)
        wait_rows(1, 0)

        def advance(message, carry):
            @pl.when(message + ON < messages)
            def _():
                pass_on(message + ON)

            @pl.when(message + AHEAD < messages)
            def _():
                send_term(message + AHEAD)

            @pl.when(message == 2)
            def _():
                wait_rows(1, 1)
                far_copy(1).start()

            @pl.when(message == 3)
            def _():
                wait_rows(1, 2)

            keep_term(message)
            return carry

        lax.fori_loop(0, messages, advance, 0)

        whole(final, send_sems.at[10])
        whole(sent, send_sems.at[9])
        whole(attended.at[0], send_sems.at[8])
        whole(attended.at[0, 0], send_sems.at[7])
        whole(w_far.at[pl.ds(0, share)], send_sems.at[5])
        whole(kv_all.at[:, pl.ds(0, (seq_count - 1) * tokens)], send_sems.at[0])
        whole(out_ref.at[:, pl.ds(0, 3 * quarter)], f_sems.at[1])

    whole(q_send.at[:, pl.ds(0, seq_count - 1)], send_sems.at[1])


def fused_device(queries, keys, values, out_weight, doc_lengths, pair_ids, block_plan):
    seq_count = lax.axis_size("seq")
    head_count = lax.axis_size("head")
    tokens, width = queries.shape
    slots = block_plan.shape[0] // seq_count
    block_rows = tokens // slots
    out_width = out_weight.shape[1]
    quarter = out_width // 4
    tiles = pick_tiles(quarter)
    tile = quarter // tiles
    half = jnp.bfloat16
    flow = pltpu.VMEM((2 * tiles, 4 * block_rows, tile), half)
    weights = pltpu.VMEM((width, quarter), half)
    in_vmem = pl.BlockSpec(memory_space=pltpu.VMEM)
    anywhere = pl.BlockSpec(memory_space=pl.ANY)
    in_smem = pl.BlockSpec(memory_space=pltpu.SMEM)
    dma = pltpu.SemaphoreType.DMA
    return pl.pallas_call(
        functools.partial(fused_kernel, seq_count, head_count),
        out_shape=jax.ShapeDtypeStruct((block_rows, out_width), half),
        in_specs=[anywhere, anywhere, anywhere, anywhere, in_vmem, in_smem, in_smem],
        out_specs=anywhere,
        scratch_shapes=[
            pltpu.VMEM((slots, block_rows, width), half),
            pltpu.VMEM(keys.shape, half),
            pltpu.VMEM(values.shape, half),
            weights,
            weights,
            pltpu.VMEM((2, seq_count * tokens, D_HEAD), half),
            pltpu.VMEM((2, seq_count, block_rows, width // 2), half),
            pltpu.VMEM((seq_count, block_rows, width // 2), half),
            pltpu.VMEM((seq_count, block_rows, width // 2), half),
            pltpu.VMEM((2, 2, 2, width // D_HEAD * block_rows, D_HEAD), half),
            pltpu.VMEM(
                (seq_count * tokens // (2 * D_HEAD), tokens, 2 * D_HEAD), jnp.float32
            ),
            pltpu.VMEM((2, 2, 2, 2, block_rows, 2 * width), half),
            flow,
            flow,
            flow,
            dma((4,)),
            dma((11,)),
            dma((4,)),
            dma((2,)),
            dma((2, 2)),
            dma((2 * tiles,)),
            dma((tiles,)),
            dma((2, 3)),
            dma((2 * tiles,)),
            dma((2,)),
        ],
        compiler_params=pltpu.CompilerParams(
            collective_id=0, has_side_effects=True, vmem_limit_bytes=60000 * 1024
        ),
    )(
        queries.reshape(slots, block_rows, width),
        keys,
        values,
        out_weight,
        pair_ids[None],
        doc_lengths,
        block_plan,
    )


def pick_device(queries, keys, values, out_weight, doc_lengths, pair_ids, block_plan):
    seq_count = lax.axis_size("seq")
    head_count = lax.axis_size("head")
    tokens, width = queries.shape
    out_width = out_weight.shape[1]
    block_rows = tokens * seq_count // block_plan.shape[0]
    fits = seq_count * tokens * tokens * 4 <= 4 * 1024 * 1024
    shape = head_count == 4 and seq_count == 8 and keys.shape[1] == 2 * D_HEAD and width % (2 * D_HEAD) == 0
    square = block_rows * head_count == tokens and block_rows % 16 == 0
    even = seq_count * tokens % (2 * D_HEAD) == 0 and width % 64 == 0
    wide = out_width % 2 == 0 and out_width // 4 % (8 * 128) == 0
    run = fused_device if fits and shape and square and even and wide else on_device
    return run(queries, keys, values, out_weight, doc_lengths, pair_ids, block_plan)


def solution(mesh):
    return jax.shard_map(
        pick_device,
        mesh=mesh,
        in_specs=(P("seq", "head"), P("seq", None), P("seq", None), P("head", None), P(), P(), P()),
        out_specs=P(("seq", "head"), None),
        check_vma=False,
    )
```

```python
import functools
import math

import jax
import jax.numpy as jnp
from jax import lax
from jax.experimental import pallas as pl
from jax.experimental.pallas import tpu as pltpu
from jax.sharding import PartitionSpec as P

D_HEAD = 128


NEGATIVE = -1e30


def token_docs(positions, doc_lengths):
    doc_ends = jnp.cumsum(doc_lengths)
    return jnp.sum((doc_ends[None, :] <= positions[:, None]).astype(jnp.int32), axis=1)


def pair_firsts(docs, pair_ids):
    doc_range = jnp.arange(pair_ids.shape[0], dtype=jnp.int32)
    own_pair = jnp.sum(jnp.where(docs[:, None] == doc_range[None, :], pair_ids[None, :], 0), axis=1)
    return jnp.sum((pair_ids[None, :] < own_pair[:, None]).astype(jnp.int32), axis=1)


def largest_divisor(total_rows, ceiling):
    return max(
        (
            candidate
            for candidate in range(1, min(total_rows, ceiling) + 1)
            if total_rows % candidate == 0
        )
    )


def attend(query_rows, positions, keys, values, doc_lengths, pair_ids):
    head_size = keys.shape[1]
    token_count = query_rows.shape[0]
    query_heads = query_rows.shape[1] // head_size
    shaped_queries = query_rows.reshape(token_count, query_heads, head_size)
    query_docs = token_docs(positions, doc_lengths)
    query_firsts = pair_firsts(query_docs, pair_ids)
    doc_range = jnp.arange(doc_lengths.shape[0], dtype=jnp.int32)
    pair_begin = jnp.sum(
        jnp.where(doc_range[None, :] < query_firsts[:, None], doc_lengths[None, :], 0), axis=1
    )
    lowest = jnp.min(pair_begin)
    highest = jnp.max(positions)
    scale = 1.0 / math.sqrt(head_size)

    def update(softmax_state, key_block, value_block, block_start):
        key_pos = block_start + jnp.arange(key_block.shape[0], dtype=jnp.int32)
        needed = (block_start <= highest) & (block_start + key_block.shape[0] > lowest)

        def compute(current):
            running_max, denominator, weighted = current
            key_docs = token_docs(key_pos, doc_lengths)
            allowed = (key_pos[None, :] <= positions[:, None]) & (
                (key_docs[None, :] == query_docs[:, None])
                | (key_docs[None, :] == query_firsts[:, None])
            )
            scores = (
                jnp.einsum(
                    "qhd,kd->hqk", shaped_queries, key_block, preferred_element_type=jnp.float32
                )
                * scale
            )
            newest = jnp.maximum(
                running_max, jnp.max(jnp.where(allowed[None], scores, NEGATIVE), axis=2)
            )
            weights = jnp.where(allowed[None], jnp.exp(scores - newest[:, :, None]), 0.0)
            factor = jnp.exp(running_max - newest)
            denominator = denominator * factor + jnp.sum(weights, axis=2)
            weighted = weighted * factor[:, :, None] + jnp.einsum(
                "hqk,kd->hqd",
                weights.astype(jnp.bfloat16),
                value_block,
                preferred_element_type=jnp.float32,
            )
            return (newest, denominator, weighted)

        def unchanged(current):
            return current

        return lax.cond(needed, compute, unchanged, softmax_state)

    initial = (
        jnp.full((query_heads, token_count), NEGATIVE, jnp.float32),
        jnp.zeros((query_heads, token_count), jnp.float32),
        jnp.zeros((query_heads, token_count, head_size), jnp.float32),
    )
    key_rows = lax.all_gather(keys, "seq", axis=0, tiled=True)
    value_rows = lax.all_gather(values, "seq", axis=0, tiled=True)
    row_total = key_rows.shape[0]
    block_rows = largest_divisor(row_total, 1024)
    block_count = row_total // block_rows
    stacked = (
        key_rows.reshape(block_count, block_rows, head_size),
        value_rows.reshape(block_count, block_rows, head_size),
        jnp.int32(0) + block_rows * jnp.arange(block_count, dtype=jnp.int32),
    )

    def advance(carried, block_item):
        return (update(carried, block_item[0], block_item[1], block_item[2]), None)

    result_state, unused_out = lax.scan(advance, initial, stacked)
    running_max, denominator, weighted = result_state
    attended = weighted / denominator[:, :, None]
    return (
        attended.transpose(1, 0, 2)
        .reshape(token_count, query_heads * head_size)
        .astype(jnp.bfloat16)
    )


def on_device(queries, keys, values, out_weight, doc_lengths, pair_ids, block_plan):
    seq_count = lax.axis_size("seq")
    my_seq = lax.axis_index("seq")
    shared_head = lax.axis_index("head") // 2
    key_rows = lax.dynamic_slice_in_dim(keys, shared_head * D_HEAD, D_HEAD, 1)
    value_rows = lax.dynamic_slice_in_dim(values, shared_head * D_HEAD, D_HEAD, 1)
    slots_here = seq_count // 2
    tok_rows = queries.shape[0]
    row_width = queries.shape[1]
    block_rows = tok_rows // slots_here
    slot_total = block_plan.shape[0]
    local_ids = my_seq * slots_here + jnp.arange(slots_here, dtype=jnp.int32)
    plan_rows = lax.dynamic_slice_in_dim(block_plan, my_seq * slots_here, slots_here, 0)
    planned_pos = (
        plan_rows[:, None] * block_rows + jnp.arange(block_rows, dtype=jnp.int32)[None, :]
    ).reshape(-1)
    slot_range = jnp.arange(slot_total, dtype=jnp.int32)
    target_slot = jnp.sum(
        jnp.where(block_plan[None, :] == local_ids[:, None], slot_range[None, :], 0), axis=1
    )
    device_range = jnp.arange(seq_count, dtype=jnp.int32)
    send_table = ((target_slot // slots_here)[:, None] == device_range[None, :]).astype(
        jnp.bfloat16
    )
    take_table = ((plan_rows // slots_here)[:, None] == device_range[None, :]).astype(jnp.bfloat16)
    blocked = queries.reshape(slots_here, block_rows, row_width)
    arrived = lax.all_to_all(
        jnp.einsum("bn,bkw->nkw", send_table, blocked, preferred_element_type=jnp.float32).astype(
            jnp.bfloat16
        ),
        "seq",
        split_axis=0,
        concat_axis=0,
        tiled=True,
    )
    chosen = jnp.einsum("bn,nkw->bkw", take_table, arrived, preferred_element_type=jnp.float32)
    attended = attend(
        chosen.astype(jnp.bfloat16).reshape(tok_rows, row_width),
        planned_pos,
        key_rows,
        value_rows,
        doc_lengths,
        pair_ids,
    )
    return lax.psum_scatter(
        jnp.dot(attended, out_weight, preferred_element_type=jnp.float32).astype(jnp.bfloat16),
        "head",
        scatter_dimension=0,
        tiled=True,
    )


FAR = 1e9
AHEAD = 5
EARLY = 4
ON = 11


def pick_tiles(width):
    return max(c for c in (1, 2, 4, 8) if width % (c * 128) == 0)


def fused_kernel(
    seq_count,
    head_count,
    queries_hbm,
    keys_hbm,
    values_hbm,
    weight_hbm,
    pairs_ref,
    lens_ref,
    plan_ref,
    out_ref,
    queries_ref,
    keys_ref,
    values_ref,
    w_own,
    w_far,
    kv_all,
    q_send,
    q_recv_a,
    q_recv_b,
    q_heads,
    bias,
    attended,
    sent,
    arrived,
    final,
    load_sems,
    send_sems,
    kv_sems,
    q_sems,
    qz_sems,
    wz_sems,
    near_sems,
    a_sems,
    b_sems,
    f_sems,
):
    q_recv = (q_recv_a, q_recv_b)
    me = lax.axis_index("seq")
    rank = lax.axis_index("head")
    core = lax.rem(me, 2)
    partner = me + 1 - 2 * core
    along_x = me + 2 - 4 * lax.rem(me // 2, 2)
    along_y = lax.rem(me + seq_count // 2, seq_count)
    quad = lax.rem(me, 4)
    base = me - quad
    side = quad // 2
    low = rank < head_count // 2
    inner = (rank > 0) & (rank < head_count - 1)
    mate = rank + 1 - 2 * lax.rem(rank, 2)
    across = head_count - 1 - rank
    slots, block_rows, width = queries_ref.shape
    tokens = slots * block_rows
    seq_len = seq_count * tokens
    pair_heads = width // (2 * D_HEAD)
    pair_width = pair_heads * D_HEAD
    shared = head_count // (keys_ref.shape[1] // D_HEAD)
    messages, rows_all, tile = sent.shape
    tiles = messages // 2
    quarter = tiles * tile
    share = width // (seq_count // 4)
    piece = share // 2

    def slot_at(place):
        at = (head_count - 1, head_count // 2, 0, 1)[place]
        return jnp.where(low, at, head_count - 1 - at)

    def piece_rows(device, at):
        return pl.ds(
            pl.multiple_of((device // 4) * share + lax.rem(at, 2) * piece, piece), piece
        )

    def tile_cols(at):
        return pl.ds(pl.multiple_of(at * tile, tile), tile)

    def out_cols(owner, at):
        return pl.ds(pl.multiple_of(owner * quarter + at * tile, tile), tile)

    def order(message):
        message = jnp.int32(message)
        last = message == messages - 1
        late = (message >= messages - 4) & jnp.logical_not(last)
        odd = lax.rem(message, 2) == 1
        other = late | ((message >= 3) & odd & jnp.logical_not(last))
        at = jnp.where(odd, (message - 3) // 2, (message + 2) // 2)
        at = jnp.where(late, message - tiles + 1, jnp.where(message < 3, message, at))
        return jnp.where(last, tiles - 1, at), other

    own_copy = pltpu.make_async_copy(
        weight_hbm.at[:, pl.ds(pl.multiple_of(quad * quarter, quarter), quarter)],
        w_own,
        load_sems.at[0],
    )
    queries_copy = pltpu.make_async_copy(queries_hbm, queries_ref, load_sems.at[1])
    kv_col = pl.ds(pl.multiple_of((rank // shared) * D_HEAD, D_HEAD), D_HEAD)
    mine = pl.ds(pl.multiple_of(me * tokens, tokens), tokens)
    keys_copy = pltpu.make_async_copy(keys_hbm, keys_ref, load_sems.at[2])
    values_copy = pltpu.make_async_copy(values_hbm, values_ref, load_sems.at[3])

    barrier = pltpu.get_barrier_semaphore()
    for step in range(1, seq_count):
        pl.semaphore_signal(barrier, inc=1, device_id={"seq": lax.rem(me + step, seq_count)})

    for place in range(4):
        pl.semaphore_signal(barrier, inc=1, device_id={"seq": base + place, "head": mate})

    @pl.when(inner)
    def _():
        pl.semaphore_signal(barrier, inc=1, device_id={"head": across})

    queries_copy.start()

    @pl.when(inner)
    def _():
        keys_copy.start()
        values_copy.start()
        own_copy.start()
        keys_copy.wait()
        values_copy.wait()
        kv_all[0, mine] = keys_ref[:, kv_col]
        kv_all[1, mine] = values_ref[:, kv_col]

    queries_copy.wait()
    for other in range(seq_count):
        local = jnp.int32(0)
        for slot in range(slots):
            offset = plan_ref[other * slots + slot] - me * slots
            local = local + jnp.where((offset >= 0) & (offset < slots), offset, 0)
        block = queries_ref[local]
        for part in range(2):
            q_send[part, other] = block[:, part * pair_width : (part + 1) * pair_width]
    for part in range(2):
        q_recv[part][me] = q_send[part, me]

    pl.semaphore_wait(barrier, seq_count + 3 + jnp.where(inner, 1, 0))

    def kv_copy(peer, slot, sem):
        rows = pl.ds(pl.multiple_of(slot * tokens, tokens), tokens)
        return pltpu.make_async_remote_copy(
            src_ref=kv_all.at[:, rows],
            dst_ref=kv_all.at[:, rows],
            send_sem=send_sems.at[0],
            recv_sem=kv_sems.at[sem],
            device_id={"seq": peer},
        )

    def q_copy(part, peer, slot):
        return pltpu.make_async_remote_copy(
            src_ref=q_send.at[part, peer],
            dst_ref=q_recv[part].at[slot],
            send_sem=send_sems.at[1],
            recv_sem=q_sems.at[part],
            device_id={"seq": peer},
        )

    def qz_copy(part, kept):
        return pltpu.make_async_remote_copy(
            src_ref=q_heads.at[0, part, kept],
            dst_ref=q_heads.at[1, part, kept],
            send_sem=send_sems.at[2],
            recv_sem=qz_sems.at[part, kept],
            device_id={"head": mate},
        )

    def wz_copy(at):
        rows = piece_rows(me, at)
        return pltpu.make_async_remote_copy(
            src_ref=weight_hbm.at[rows, out_cols(quad, at // 2)],
            dst_ref=w_far.at[rows, tile_cols(at // 2)],
            send_sem=send_sems.at[3],
            recv_sem=wz_sems.at[at],
            device_id={"head": mate},
        )

    def relay(at):
        rows = piece_rows(me, at)
        return pltpu.make_async_remote_copy(
            src_ref=w_far.at[rows, tile_cols(at // 2)],
            dst_ref=w_far.at[rows, tile_cols(at // 2)],
            send_sem=send_sems.at[5],
            recv_sem=near_sems.at[at // 2],
            device_id={"seq": along_y},
        )

    def a_copy(kept, group, kind, peer):
        cols = pl.ds(group * width, width)
        return pltpu.make_async_remote_copy(
            src_ref=attended.at[kept, side, core, :, :, cols],
            dst_ref=attended.at[kept, side, core, :, :, cols],
            send_sem=send_sems.at[8],
            recv_sem=a_sems.at[kept, kind],
            device_id={"seq": peer},
        )

    def far_copy(kept):
        return pltpu.make_async_remote_copy(
            src_ref=attended.at[kept, 1 - side, core],
            dst_ref=attended.at[kept, 1 - side, core],
            send_sem=send_sems.at[7],
            recv_sem=a_sems.at[kept, 2],
            device_id={"seq": partner},
        )

    def core_rows(which):
        return pl.ds(pl.multiple_of(which * 2 * block_rows, block_rows), 2 * block_rows)

    def start_copy(which):
        return pltpu.make_async_remote_copy(
            src_ref=sent.at[0, core_rows(which)],
            dst_ref=arrived.at[0, core_rows(which)],
            send_sem=send_sems.at[9],
            recv_sem=b_sems.at[0],
            device_id={"head": across},
        )

    def b_copy(at):
        return pltpu.make_async_remote_copy(
            src_ref=sent.at[at],
            dst_ref=arrived.at[at],
            send_sem=send_sems.at[9],
            recv_sem=b_sems.at[at],
            device_id={"head": across},
        )

    def kind_rows(which, kind):
        return pl.ds(pl.multiple_of((2 * which + kind) * block_rows, block_rows), block_rows)

    def last_copy(kind, which):
        row = (2 * which + kind) * block_rows
        rows = pl.ds(row, block_rows)
        return pltpu.make_async_remote_copy(
            src_ref=sent.at[messages - 1, rows],
            dst_ref=arrived.at[messages - 1, rows],
            send_sem=send_sems.at[9],
            recv_sem=b_sems.at[messages - 1 + kind],
            device_id={"head": across},
        )

    def edge_copy(message, at, half, which):
        return pltpu.make_async_remote_copy(
            src_ref=final.at[message, kind_rows(which, 0)],
            dst_ref=out_ref.at[:, out_cols(quad, at)],
            send_sem=send_sems.at[10],
            recv_sem=f_sems.at[0],
            device_id={"seq": base + 2 * half + which, "head": mate},
        )

    def inner_copy(message, at, half, which):
        return pltpu.make_async_remote_copy(
            src_ref=final.at[message, kind_rows(which, 1)],
            dst_ref=out_ref.at[:, out_cols(quad, at)],
            send_sem=send_sems.at[10],
            recv_sem=f_sems.at[1],
            device_id={"seq": base + 2 * half + which},
        )

    def out_copy(message, at):
        return pltpu.make_async_copy(
            final.at[message, kind_rows(core, 1)],
            out_ref.at[:, out_cols(quad, at)],
            send_sems.at[10],
        )

    def whole(ref, sem):
        pltpu.make_async_copy(ref, ref, sem).wait()

    @pl.when(inner)
    def _():
        for step in range(2, seq_count, 2):
            peer = lax.rem(me + step, seq_count)
            kv_copy(peer, me, step // 2 - 1).start()
        kv_copy(partner, me, 3).start()

    @pl.when(jnp.logical_not(inner))
    def _():
        for at in range(EARLY):
            wz_copy(at).start()

    for part in range(2):
        for step in range(1, seq_count):
            peer = lax.rem(me + step, seq_count)
            q_copy(part, peer, me).start()

    def gather_queries(part):
        whole(q_recv[part].at[pl.ds(0, seq_count - 1)], q_sems.at[part])
        for place in range(slots):
            block = q_recv[part][plan_ref[me * slots + slot_at(place)] // slots]
            for head in range(pair_heads):
                row = ((place % 2) * pair_heads + head) * block_rows
                q_heads[0, part, place // 2, row : row + block_rows, :] = block[
                    :, head * D_HEAD : (head + 1) * D_HEAD
                ]

    @pl.when(jnp.logical_not(inner))
    def _():
        gather_queries(0)
        qz_copy(0, 0).start()
        gather_queries(1)
        qz_copy(1, 0).start()
        for at in range(EARLY, EARLY + 4):
            wz_copy(at).start()
        qz_copy(0, 1).start()
        qz_copy(1, 1).start()

        def push_next(at, carry):
            wz_copy(at).start()
            return carry

        lax.fori_loop(EARLY + 4, messages, push_next, 0)
        whole(out_ref, f_sems.at[0])
        whole(weight_hbm.at[pl.ds(0, share), pl.ds(0, quarter)], send_sems.at[3])
        whole(q_heads.at[0], send_sems.at[2])

    @pl.when(inner)
    def _():
        row = lax.broadcasted_iota(jnp.int32, (tokens, 1), 0)
        position = row
        for place in range(slots):
            shift = (plan_ref[me * slots + slot_at(place)] - place) * block_rows
            here = (row >= place * block_rows) & (row < (place + 1) * block_rows)
            position = position + jnp.where(here, shift, 0)
        position = position.astype(jnp.float32)
        docs = pairs_ref.shape[1]
        doc_at = lax.broadcasted_iota(jnp.int32, (1, docs), 1)
        starts = jnp.zeros((1, docs), jnp.int32)
        ends = jnp.zeros((1, docs), jnp.int32)
        running = jnp.int32(0)
        for doc in range(docs):
            starts = jnp.where(doc_at == doc, running, starts)
            running = running + lens_ref[doc]
            ends = jnp.where(doc_at == doc, running, ends)
        starts = starts.astype(jnp.float32)
        ends = ends.astype(jnp.float32)
        pairs = pairs_ref[...].astype(jnp.float32)
        begun = starts <= position
        own_start = jnp.max(jnp.where(begun, starts, 0.0), axis=1, keepdims=True)
        own_pair = jnp.max(jnp.where(begun, pairs, 0.0), axis=1, keepdims=True)
        same = pairs == own_pair
        first_start = jnp.min(jnp.where(same, starts, FAR), axis=1, keepdims=True)
        first_end = jnp.min(jnp.where(same, ends, FAR), axis=1, keepdims=True)
        key_width = 2 * D_HEAD
        parts = seq_len // key_width
        for part in range(parts):
            key_pos = (
                lax.broadcasted_iota(jnp.int32, (tokens, key_width), 1) + part * key_width
            ).astype(jnp.float32)
            seen = (key_pos <= position) & (
                (key_pos >= own_start) | ((key_pos >= first_start) & (key_pos < first_end))
            )
            bias[part] = jnp.where(seen, 0.0, NEGATIVE)

        for step in range(2, seq_count, 2):
            source = lax.rem(me + seq_count - step, seq_count)
            kv_copy(partner, source, step // 2 - 1).wait_recv()
            kv_copy(partner, source, 3).start()

        def pass_on(at):
            wz_copy(at).wait_recv()
            relay(at).start()

        def complete(at):
            whole(w_far.at[pl.ds(0, share), tile_cols(at)], near_sems.at[at])

        pass_on(0)
        pass_on(1)
        gather_queries(0)
        pass_on(2)
        whole(kv_all.at[:, pl.ds(0, seq_count // 2 * tokens)], kv_sems.at[3])

        scale = math.log2(math.e) / math.sqrt(D_HEAD)

        def unit(group, part, kept):
            rows_q = q_heads[group, part, kept]
            scores = []
            for block in range(parts):
                masks = []
                for kind in range(2):
                    rows_at = (2 * kept + kind) * block_rows
                    masks += [bias[block, rows_at : rows_at + block_rows, :]] * pair_heads
                scores.append(
                    lax.dot_general(
                        rows_q,
                        kv_all[0, block * key_width : (block + 1) * key_width],
                        (((1,), (1,)), ((), ())),
                        preferred_element_type=jnp.float32,
                    )
                    * scale
                    + jnp.concatenate(masks, axis=0)
                )
            top = functools.reduce(jnp.maximum, scores)
            top = jnp.max(top, axis=1, keepdims=True)
            total = jnp.zeros((2 * pair_heads * block_rows, key_width), jnp.float32)
            summed = jnp.zeros((2 * pair_heads * block_rows, D_HEAD), jnp.float32)
            for block in range(parts):
                weights = jnp.exp2(scores[block] - top)
                total = total + weights
                summed = summed + jnp.dot(
                    weights.astype(jnp.bfloat16),
                    kv_all[1, block * key_width : (block + 1) * key_width],
                    preferred_element_type=jnp.float32,
                )
            total = jnp.sum(total, axis=1, keepdims=True)
            result = (summed / total).astype(jnp.bfloat16)
            for kind in range(2):
                for head in range(pair_heads):
                    row = (kind * pair_heads + head) * block_rows
                    at = ((group * 2 + part) * pair_heads + head) * D_HEAD
                    attended[kept, side, core, kind, :, pl.ds(pl.multiple_of(at, D_HEAD), D_HEAD)] = (
                        result[row : row + block_rows]
                    )

        def product(rows_a, at):
            return jnp.dot(
                rows_a[:, :width], w_own[:, tile_cols(at)], preferred_element_type=jnp.float32
            ) + jnp.dot(
                rows_a[:, width:], w_far[:, tile_cols(at)], preferred_element_type=jnp.float32
            )

        def half_term(which):
            rows_a = attended[0, side, which].reshape(2 * block_rows, 2 * width)
            sent[0, core_rows(which)] = product(rows_a, 0).astype(jnp.bfloat16)
            start_copy(which).start()

        def term(kept, half, at):
            return product(attended[kept, half].reshape(rows_all, 2 * width), at)

        def send_term(message):
            at, other = order(message)

            @pl.when(other == (at == tiles - 1))
            def _():
                complete(at)

            half = jnp.where(other, 1 - side, side)
            sent[message] = term(0, half, at).astype(jnp.bfloat16)
            b_copy(message).start()

        def send_last():
            message = messages - 1
            sent[message] = term(0, side, tiles - 1).astype(jnp.bfloat16)
            for kind in range(2):
                for which in range(2):
                    last_copy(kind, which).start()

        def keep_last():
            message = messages - 1
            at = tiles - 1
            mixed = term(1, side, at)
            for kind in range(2):
                whole(arrived.at[message, core_rows(0)], b_sems.at[message + kind])
                for which in range(2):
                    row = (2 * which + kind) * block_rows
                    rows = slice(row, row + block_rows)
                    final[message, rows] = (
                        mixed[rows] + arrived[message, rows].astype(jnp.float32)
                    ).astype(jnp.bfloat16)
                    if kind == 0:
                        edge_copy(message, at, side, which).start()
            inner_copy(message, at, side, 1 - core).start()
            out_copy(message, at).start()

        def keep_term(message):
            at, other = order(message)
            half = jnp.where(other, 1 - side, side)
            mixed = term(1, half, at)
            b_copy(message).wait_recv()
            final[message] = (mixed + arrived[message].astype(jnp.float32)).astype(jnp.bfloat16)
            edge_copy(message, at, half, 0).start()
            edge_copy(message, at, half, 1).start()
            inner_copy(message, at, half, 1 - core).start()

            @pl.when(other)
            def _():
                inner_copy(message, at, half, core).start()

            @pl.when(jnp.logical_not(other))
            def _():
                out_copy(message, at).start()

        def share_out(kept, group):
            a_copy(kept, group, 1, along_x).start()
            a_copy(kept, group, 0, partner).start()

        def wait_rows(kept, kind):
            whole(attended.at[kept, 0, 0], a_sems.at[kept, kind])

        def sent_unit(item, carry):
            @pl.when(item == 1)
            def _():
                gather_queries(1)
                pass_on(3)

            @pl.when(item >= 2)
            def _():
                qz_copy(item - 2, 0).wait_recv()

            unit(item // 2, lax.rem(item, 2), 0)

            @pl.when(item == 1)
            def _():
                share_out(0, 0)

            return carry

        def kept_unit(item, carry):
            @pl.when(item >= 2)
            def _():
                qz_copy(item - 2, 1).wait_recv()

            unit(item // 2, lax.rem(item, 2), 1)
            return carry

        lax.fori_loop(0, 4, sent_unit, 0)
        share_out(0, 1)
        own_copy.wait()
        pass_on(4)
        complete(0)
        half_term(core)
        wait_rows(0, 0)
        half_term(1 - core)
        pass_on(5)
        lax.fori_loop(0, 2, kept_unit, 0)
        share_out(1, 0)
        pass_on(6)
        send_term(1)
        wait_rows(0, 1)
        far_copy(0).start()
        pass_on(7)
        send_term(2)
        wait_rows(0, 2)
        send_term(3)
        pass_on(8)
        lax.fori_loop(2, 4, kept_unit, 0)
        share_out(1, 1)
        pass_on(9)
        send_term(4)
        pass_on(10)
        wait_rows(1, 0)

        def advance(message, carry):
            @pl.when(message + ON < messages)
            def _():
                pass_on(message + ON)

            @pl.when(message + AHEAD < messages - 1)
            def _():
                send_term(message + AHEAD)

            @pl.when(message + AHEAD == messages - 1)
            def _():
                send_last()

            @pl.when(message == 2)
            def _():
                wait_rows(1, 1)
                far_copy(1).start()

            @pl.when(message == 3)
            def _():
                wait_rows(1, 2)

            keep_term(message)
            return carry

        lax.fori_loop(0, messages - 1, advance, 0)
        keep_last()

        whole(final, send_sems.at[10])
        whole(sent, send_sems.at[9])
        whole(attended.at[0], send_sems.at[8])
        whole(attended.at[0, 0], send_sems.at[7])
        whole(w_far.at[pl.ds(0, share)], send_sems.at[5])
        whole(kv_all.at[:, pl.ds(0, (seq_count - 1) * tokens)], send_sems.at[0])
        whole(out_ref.at[:, pl.ds(0, 3 * quarter)], f_sems.at[1])

    whole(q_send.at[:, pl.ds(0, seq_count - 1)], send_sems.at[1])


def fused_device(queries, keys, values, out_weight, doc_lengths, pair_ids, block_plan):
    seq_count = lax.axis_size("seq")
    head_count = lax.axis_size("head")
    tokens, width = queries.shape
    slots = block_plan.shape[0] // seq_count
    block_rows = tokens // slots
    out_width = out_weight.shape[1]
    quarter = out_width // 4
    tiles = pick_tiles(quarter)
    tile = quarter // tiles
    half = jnp.bfloat16
    flow = pltpu.VMEM((2 * tiles, 4 * block_rows, tile), half)
    weights = pltpu.VMEM((width, quarter), half)
    in_vmem = pl.BlockSpec(memory_space=pltpu.VMEM)
    anywhere = pl.BlockSpec(memory_space=pl.ANY)
    in_smem = pl.BlockSpec(memory_space=pltpu.SMEM)
    dma = pltpu.SemaphoreType.DMA
    return pl.pallas_call(
        functools.partial(fused_kernel, seq_count, head_count),
        out_shape=pltpu.VMEM((block_rows, out_width), half),
        in_specs=[anywhere, anywhere, anywhere, anywhere, in_vmem, in_smem, in_smem],
        out_specs=in_vmem,
        scratch_shapes=[
            pltpu.VMEM((slots, block_rows, width), half),
            pltpu.VMEM(keys.shape, half),
            pltpu.VMEM(values.shape, half),
            weights,
            weights,
            pltpu.VMEM((2, seq_count * tokens, D_HEAD), half),
            pltpu.VMEM((2, seq_count, block_rows, width // 2), half),
            pltpu.VMEM((seq_count, block_rows, width // 2), half),
            pltpu.VMEM((seq_count, block_rows, width // 2), half),
            pltpu.VMEM((2, 2, 2, width // D_HEAD * block_rows, D_HEAD), half),
            pltpu.VMEM(
                (seq_count * tokens // (2 * D_HEAD), tokens, 2 * D_HEAD), jnp.float32
            ),
            pltpu.VMEM((2, 2, 2, 2, block_rows, 2 * width), half),
            flow,
            flow,
            flow,
            dma((4,)),
            dma((11,)),
            dma((4,)),
            dma((2,)),
            dma((2, 2)),
            dma((2 * tiles,)),
            dma((tiles,)),
            dma((2, 3)),
            dma((2 * tiles + 1,)),
            dma((2,)),
        ],
        compiler_params=pltpu.CompilerParams(
            collective_id=0, has_side_effects=True, vmem_limit_bytes=60000 * 1024
        ),
    )(
        queries.reshape(slots, block_rows, width),
        keys,
        values,
        out_weight,
        pair_ids[None],
        doc_lengths,
        block_plan,
    )


def pick_device(queries, keys, values, out_weight, doc_lengths, pair_ids, block_plan):
    seq_count = lax.axis_size("seq")
    head_count = lax.axis_size("head")
    tokens, width = queries.shape
    out_width = out_weight.shape[1]
    block_rows = tokens * seq_count // block_plan.shape[0]
    fits = seq_count * tokens * tokens * 4 <= 4 * 1024 * 1024
    shape = head_count == 4 and seq_count == 8 and keys.shape[1] == 2 * D_HEAD and width % (2 * D_HEAD) == 0
    square = block_rows * head_count == tokens and block_rows % 16 == 0
    even = seq_count * tokens % (2 * D_HEAD) == 0 and width % 64 == 0
    wide = out_width % 2 == 0 and out_width // 4 % (8 * 128) == 0
    run = fused_device if fits and shape and square and even and wide else on_device
    return run(queries, keys, values, out_weight, doc_lengths, pair_ids, block_plan)


def solution(mesh):
    return jax.shard_map(
        pick_device,
        mesh=mesh,
        in_specs=(P("seq", "head"), P("seq", None), P("seq", None), P("head", None), P(), P(), P()),
        out_specs=P(("seq", "head"), None),
        check_vma=False,
    )
```

```python
import functools
import math

import jax
import jax.numpy as jnp
from jax import lax
from jax.experimental import pallas as pl
from jax.experimental.pallas import tpu as pltpu
from jax.sharding import PartitionSpec as P

D_HEAD = 128


NEGATIVE = -1e30


def token_docs(positions, doc_lengths):
    doc_ends = jnp.cumsum(doc_lengths)
    return jnp.sum((doc_ends[None, :] <= positions[:, None]).astype(jnp.int32), axis=1)


def pair_firsts(docs, pair_ids):
    doc_range = jnp.arange(pair_ids.shape[0], dtype=jnp.int32)
    own_pair = jnp.sum(jnp.where(docs[:, None] == doc_range[None, :], pair_ids[None, :], 0), axis=1)
    return jnp.sum((pair_ids[None, :] < own_pair[:, None]).astype(jnp.int32), axis=1)


def largest_divisor(total_rows, ceiling):
    return max(
        (
            candidate
            for candidate in range(1, min(total_rows, ceiling) + 1)
            if total_rows % candidate == 0
        )
    )


def attend(query_rows, positions, keys, values, doc_lengths, pair_ids):
    head_size = keys.shape[1]
    token_count = query_rows.shape[0]
    query_heads = query_rows.shape[1] // head_size
    shaped_queries = query_rows.reshape(token_count, query_heads, head_size)
    query_docs = token_docs(positions, doc_lengths)
    query_firsts = pair_firsts(query_docs, pair_ids)
    doc_range = jnp.arange(doc_lengths.shape[0], dtype=jnp.int32)
    pair_begin = jnp.sum(
        jnp.where(doc_range[None, :] < query_firsts[:, None], doc_lengths[None, :], 0), axis=1
    )
    lowest = jnp.min(pair_begin)
    highest = jnp.max(positions)
    scale = 1.0 / math.sqrt(head_size)

    def update(softmax_state, key_block, value_block, block_start):
        key_pos = block_start + jnp.arange(key_block.shape[0], dtype=jnp.int32)
        needed = (block_start <= highest) & (block_start + key_block.shape[0] > lowest)

        def compute(current):
            running_max, denominator, weighted = current
            key_docs = token_docs(key_pos, doc_lengths)
            allowed = (key_pos[None, :] <= positions[:, None]) & (
                (key_docs[None, :] == query_docs[:, None])
                | (key_docs[None, :] == query_firsts[:, None])
            )
            scores = (
                jnp.einsum(
                    "qhd,kd->hqk", shaped_queries, key_block, preferred_element_type=jnp.float32
                )
                * scale
            )
            newest = jnp.maximum(
                running_max, jnp.max(jnp.where(allowed[None], scores, NEGATIVE), axis=2)
            )
            weights = jnp.where(allowed[None], jnp.exp(scores - newest[:, :, None]), 0.0)
            factor = jnp.exp(running_max - newest)
            denominator = denominator * factor + jnp.sum(weights, axis=2)
            weighted = weighted * factor[:, :, None] + jnp.einsum(
                "hqk,kd->hqd",
                weights.astype(jnp.bfloat16),
                value_block,
                preferred_element_type=jnp.float32,
            )
            return (newest, denominator, weighted)

        def unchanged(current):
            return current

        return lax.cond(needed, compute, unchanged, softmax_state)

    initial = (
        jnp.full((query_heads, token_count), NEGATIVE, jnp.float32),
        jnp.zeros((query_heads, token_count), jnp.float32),
        jnp.zeros((query_heads, token_count, head_size), jnp.float32),
    )
    key_rows = lax.all_gather(keys, "seq", axis=0, tiled=True)
    value_rows = lax.all_gather(values, "seq", axis=0, tiled=True)
    row_total = key_rows.shape[0]
    block_rows = largest_divisor(row_total, 1024)
    block_count = row_total // block_rows
    stacked = (
        key_rows.reshape(block_count, block_rows, head_size),
        value_rows.reshape(block_count, block_rows, head_size),
        jnp.int32(0) + block_rows * jnp.arange(block_count, dtype=jnp.int32),
    )

    def advance(carried, block_item):
        return (update(carried, block_item[0], block_item[1], block_item[2]), None)

    result_state, unused_out = lax.scan(advance, initial, stacked)
    running_max, denominator, weighted = result_state
    attended = weighted / denominator[:, :, None]
    return (
        attended.transpose(1, 0, 2)
        .reshape(token_count, query_heads * head_size)
        .astype(jnp.bfloat16)
    )


def on_device(queries, keys, values, out_weight, doc_lengths, pair_ids, block_plan):
    seq_count = lax.axis_size("seq")
    my_seq = lax.axis_index("seq")
    shared_head = lax.axis_index("head") // 2
    key_rows = lax.dynamic_slice_in_dim(keys, shared_head * D_HEAD, D_HEAD, 1)
    value_rows = lax.dynamic_slice_in_dim(values, shared_head * D_HEAD, D_HEAD, 1)
    slots_here = seq_count // 2
    tok_rows = queries.shape[0]
    row_width = queries.shape[1]
    block_rows = tok_rows // slots_here
    slot_total = block_plan.shape[0]
    local_ids = my_seq * slots_here + jnp.arange(slots_here, dtype=jnp.int32)
    plan_rows = lax.dynamic_slice_in_dim(block_plan, my_seq * slots_here, slots_here, 0)
    planned_pos = (
        plan_rows[:, None] * block_rows + jnp.arange(block_rows, dtype=jnp.int32)[None, :]
    ).reshape(-1)
    slot_range = jnp.arange(slot_total, dtype=jnp.int32)
    target_slot = jnp.sum(
        jnp.where(block_plan[None, :] == local_ids[:, None], slot_range[None, :], 0), axis=1
    )
    device_range = jnp.arange(seq_count, dtype=jnp.int32)
    send_table = ((target_slot // slots_here)[:, None] == device_range[None, :]).astype(
        jnp.bfloat16
    )
    take_table = ((plan_rows // slots_here)[:, None] == device_range[None, :]).astype(jnp.bfloat16)
    blocked = queries.reshape(slots_here, block_rows, row_width)
    arrived = lax.all_to_all(
        jnp.einsum("bn,bkw->nkw", send_table, blocked, preferred_element_type=jnp.float32).astype(
            jnp.bfloat16
        ),
        "seq",
        split_axis=0,
        concat_axis=0,
        tiled=True,
    )
    chosen = jnp.einsum("bn,nkw->bkw", take_table, arrived, preferred_element_type=jnp.float32)
    attended = attend(
        chosen.astype(jnp.bfloat16).reshape(tok_rows, row_width),
        planned_pos,
        key_rows,
        value_rows,
        doc_lengths,
        pair_ids,
    )
    return lax.psum_scatter(
        jnp.dot(attended, out_weight, preferred_element_type=jnp.float32).astype(jnp.bfloat16),
        "head",
        scatter_dimension=0,
        tiled=True,
    )


FAR = 1e9
AHEAD = 5
EARLY = 4
ON = 11


def pick_tiles(width):
    return max(c for c in (1, 2, 4, 8) if width % (c * 128) == 0)


def fused_kernel(
    seq_count,
    head_count,
    queries_hbm,
    keys_hbm,
    values_hbm,
    weight_hbm,
    pairs_ref,
    lens_ref,
    plan_ref,
    out_ref,
    queries_ref,
    keys_ref,
    values_ref,
    w_own,
    w_far,
    kv_all,
    q_send,
    q_recv_a,
    q_recv_b,
    q_heads,
    bias,
    attended,
    sent,
    arrived,
    final,
    load_sems,
    send_sems,
    kv_sems,
    q_sems,
    qz_sems,
    wz_sems,
    near_sems,
    a_sems,
    b_sems,
    f_sems,
):
    q_recv = (q_recv_a, q_recv_b)
    me = lax.axis_index("seq")
    rank = lax.axis_index("head")
    core = lax.rem(me, 2)
    partner = me + 1 - 2 * core
    along_x = me + 2 - 4 * lax.rem(me // 2, 2)
    along_y = lax.rem(me + seq_count // 2, seq_count)
    first = along_y
    second = along_x
    corner = along_x + along_y - me
    quad = lax.rem(me, 4)
    base = me - quad
    side = quad // 2
    low = rank < head_count // 2
    inner = (rank > 0) & (rank < head_count - 1)
    mate = rank + 1 - 2 * lax.rem(rank, 2)
    across = head_count - 1 - rank
    slots, block_rows, width = queries_ref.shape
    tokens = slots * block_rows
    seq_len = seq_count * tokens
    pair_heads = width // (2 * D_HEAD)
    pair_width = pair_heads * D_HEAD
    shared = head_count // (keys_ref.shape[1] // D_HEAD)
    messages, rows_all, tile = sent.shape
    tiles = messages // 2
    quarter = tiles * tile
    share = width // (seq_count // 4)
    piece = share // 2

    def slot_at(place):
        at = (head_count - 1, head_count // 2, 0, 1)[place]
        return jnp.where(low, at, head_count - 1 - at)

    def piece_rows(device, at):
        return pl.ds(
            pl.multiple_of((device // 4) * share + lax.rem(at, 2) * piece, piece), piece
        )

    def tile_cols(at):
        return pl.ds(pl.multiple_of(at * tile, tile), tile)

    def out_cols(owner, at):
        return pl.ds(pl.multiple_of(owner * quarter + at * tile, tile), tile)

    def order(message):
        message = jnp.int32(message)
        late = message == messages - 3
        odd = lax.rem(message, 2) == 1
        other = late | ((message >= 2) & jnp.logical_not(odd))
        at = jnp.where(odd, (message + 1) // 2, (message - 2) // 2)
        at = jnp.where(late, tiles - 2, jnp.where(message == 0, 0, at))
        return at, other

    own_copy = pltpu.make_async_copy(
        weight_hbm.at[:, pl.ds(pl.multiple_of(quad * quarter, quarter), quarter)],
        w_own,
        load_sems.at[0],
    )
    queries_copy = pltpu.make_async_copy(queries_hbm, queries_ref, load_sems.at[1])
    kv_col = pl.ds(pl.multiple_of((rank // shared) * D_HEAD, D_HEAD), D_HEAD)
    mine = pl.ds(pl.multiple_of(me * tokens, tokens), tokens)
    keys_copy = pltpu.make_async_copy(keys_hbm, keys_ref, load_sems.at[2])
    values_copy = pltpu.make_async_copy(values_hbm, values_ref, load_sems.at[3])

    barrier = pltpu.get_barrier_semaphore()
    for step in range(1, seq_count):
        pl.semaphore_signal(barrier, inc=1, device_id={"seq": lax.rem(me + step, seq_count)})

    for place in range(4):
        pl.semaphore_signal(barrier, inc=1, device_id={"seq": base + place, "head": mate})

    @pl.when(inner)
    def _():
        pl.semaphore_signal(barrier, inc=1, device_id={"head": across})

    queries_copy.start()

    @pl.when(inner)
    def _():
        keys_copy.start()
        values_copy.start()
        own_copy.start()
        keys_copy.wait()
        values_copy.wait()
        kv_all[0, mine] = keys_ref[:, kv_col]
        kv_all[1, mine] = values_ref[:, kv_col]

    queries_copy.wait()
    for other in range(seq_count):
        local = jnp.int32(0)
        for slot in range(slots):
            offset = plan_ref[other * slots + slot] - me * slots
            local = local + jnp.where((offset >= 0) & (offset < slots), offset, 0)
        block = queries_ref[local]
        for part in range(2):
            q_send[part, other] = block[:, part * pair_width : (part + 1) * pair_width]
    for part in range(2):
        q_recv[part][me] = q_send[part, me]

    pl.semaphore_wait(barrier, seq_count + 3 + jnp.where(inner, 1, 0))

    def kv_copy(peer, slot, sem):
        rows = pl.ds(pl.multiple_of(slot * tokens, tokens), tokens)
        return pltpu.make_async_remote_copy(
            src_ref=kv_all.at[:, rows],
            dst_ref=kv_all.at[:, rows],
            send_sem=send_sems.at[0],
            recv_sem=kv_sems.at[sem],
            device_id={"seq": peer},
        )

    def q_copy(part, peer, slot):
        return pltpu.make_async_remote_copy(
            src_ref=q_send.at[part, peer],
            dst_ref=q_recv[part].at[slot],
            send_sem=send_sems.at[1],
            recv_sem=q_sems.at[part],
            device_id={"seq": peer},
        )

    def qz_copy(part, kept):
        return pltpu.make_async_remote_copy(
            src_ref=q_heads.at[0, part, kept],
            dst_ref=q_heads.at[1, part, kept],
            send_sem=send_sems.at[2],
            recv_sem=qz_sems.at[part, kept],
            device_id={"head": mate},
        )

    def wz_copy(at):
        rows = piece_rows(me, at)
        return pltpu.make_async_remote_copy(
            src_ref=weight_hbm.at[rows, out_cols(quad, at // 2)],
            dst_ref=w_far.at[rows, tile_cols(at // 2)],
            send_sem=send_sems.at[3],
            recv_sem=wz_sems.at[at],
            device_id={"head": mate},
        )

    def relay(at):
        rows = piece_rows(me, at)
        return pltpu.make_async_remote_copy(
            src_ref=w_far.at[rows, tile_cols(at // 2)],
            dst_ref=w_far.at[rows, tile_cols(at // 2)],
            send_sem=send_sems.at[5],
            recv_sem=near_sems.at[at // 2],
            device_id={"seq": along_y},
        )

    def a_copy(kept, item, kind, peer):
        cols = pl.ds(pl.multiple_of(item * pair_width, pair_width), pair_width)
        return pltpu.make_async_remote_copy(
            src_ref=attended.at[kept, side, core, :, :, cols],
            dst_ref=attended.at[kept, side, core, :, :, cols],
            send_sem=send_sems.at[8],
            recv_sem=a_sems.at[kept, kind],
            device_id={"seq": peer},
        )

    def far_copy(kept):
        return pltpu.make_async_remote_copy(
            src_ref=attended.at[kept, 1 - side, core],
            dst_ref=attended.at[kept, 1 - side, core],
            send_sem=send_sems.at[7],
            recv_sem=a_sems.at[kept, 2],
            device_id={"seq": partner},
        )

    def core_rows(which):
        return pl.ds(pl.multiple_of(which * 2 * block_rows, block_rows), 2 * block_rows)

    def start_copy(which):
        return pltpu.make_async_remote_copy(
            src_ref=sent.at[0, core_rows(which)],
            dst_ref=arrived.at[0, core_rows(which)],
            send_sem=send_sems.at[9],
            recv_sem=b_sems.at[0],
            device_id={"head": across},
        )

    def b_copy(at):
        return pltpu.make_async_remote_copy(
            src_ref=sent.at[at],
            dst_ref=arrived.at[at],
            send_sem=send_sems.at[9],
            recv_sem=b_sems.at[at],
            device_id={"head": across},
        )

    def kind_rows(which, kind):
        return pl.ds(pl.multiple_of((2 * which + kind) * block_rows, block_rows), block_rows)

    def last_copy(message, kind, which):
        row = (2 * which + kind) * block_rows
        rows = pl.ds(row, block_rows)
        return pltpu.make_async_remote_copy(
            src_ref=sent.at[message, rows],
            dst_ref=arrived.at[message, rows],
            send_sem=send_sems.at[9],
            recv_sem=b_sems.at[message + 2 * kind],
            device_id={"head": across},
        )

    def edge_copy(message, at, half, which):
        return pltpu.make_async_remote_copy(
            src_ref=final.at[message, kind_rows(which, 0)],
            dst_ref=out_ref.at[:, out_cols(quad, at)],
            send_sem=send_sems.at[10],
            recv_sem=f_sems.at[0],
            device_id={"seq": base + 2 * half + which, "head": mate},
        )

    def inner_copy(message, at, half, which):
        return pltpu.make_async_remote_copy(
            src_ref=final.at[message, kind_rows(which, 1)],
            dst_ref=out_ref.at[:, out_cols(quad, at)],
            send_sem=send_sems.at[10],
            recv_sem=f_sems.at[1],
            device_id={"seq": base + 2 * half + which},
        )

    def out_copy(message, at):
        return pltpu.make_async_copy(
            final.at[message, kind_rows(core, 1)],
            out_ref.at[:, out_cols(quad, at)],
            send_sems.at[10],
        )

    def whole(ref, sem):
        pltpu.make_async_copy(ref, ref, sem).wait()

    @pl.when(inner)
    def _():
        kv_copy(first, me, 0).start()
        kv_copy(second, me, 1).start()
        kv_copy(partner, me, 3).start()

        @pl.when(core == 0)
        def _():
            kv_copy(corner, me, 2).start()

    @pl.when(jnp.logical_not(inner))
    def _():
        for at in range(EARLY):
            wz_copy(at).start()

    def send_queries(part):
        for step in range(1, seq_count):
            peer = lax.rem(me + step, seq_count)
            q_copy(part, peer, me).start()

    send_queries(0)

    @pl.when(jnp.logical_not(inner) | (core == 0))
    def _():
        send_queries(1)

    def gather_queries(part):
        whole(q_recv[part].at[pl.ds(0, seq_count - 1)], q_sems.at[part])
        for place in range(slots):
            block = q_recv[part][plan_ref[me * slots + slot_at(place)] // slots]
            for head in range(pair_heads):
                row = ((place % 2) * pair_heads + head) * block_rows
                q_heads[0, part, place // 2, row : row + block_rows, :] = block[
                    :, head * D_HEAD : (head + 1) * D_HEAD
                ]

    @pl.when(jnp.logical_not(inner))
    def _():
        gather_queries(0)
        qz_copy(0, 0).start()
        gather_queries(1)
        qz_copy(1, 0).start()
        for at in range(EARLY, EARLY + 4):
            wz_copy(at).start()
        qz_copy(0, 1).start()
        qz_copy(1, 1).start()

        def push_next(at, carry):
            wz_copy(at).start()
            return carry

        lax.fori_loop(EARLY + 4, messages, push_next, 0)
        whole(out_ref, f_sems.at[0])
        whole(weight_hbm.at[pl.ds(0, share), pl.ds(0, quarter)], send_sems.at[3])
        whole(q_heads.at[0], send_sems.at[2])

    @pl.when(inner)
    def _():
        row = lax.broadcasted_iota(jnp.int32, (tokens, 1), 0)
        position = row
        for place in range(slots):
            shift = (plan_ref[me * slots + slot_at(place)] - place) * block_rows
            here = (row >= place * block_rows) & (row < (place + 1) * block_rows)
            position = position + jnp.where(here, shift, 0)
        position = position.astype(jnp.float32)
        docs = pairs_ref.shape[1]
        doc_at = lax.broadcasted_iota(jnp.int32, (1, docs), 1)
        starts = jnp.zeros((1, docs), jnp.int32)
        ends = jnp.zeros((1, docs), jnp.int32)
        running = jnp.int32(0)
        for doc in range(docs):
            starts = jnp.where(doc_at == doc, running, starts)
            running = running + lens_ref[doc]
            ends = jnp.where(doc_at == doc, running, ends)
        starts = starts.astype(jnp.float32)
        ends = ends.astype(jnp.float32)
        pairs = pairs_ref[...].astype(jnp.float32)
        begun = starts <= position
        own_start = jnp.max(jnp.where(begun, starts, 0.0), axis=1, keepdims=True)
        own_pair = jnp.max(jnp.where(begun, pairs, 0.0), axis=1, keepdims=True)
        same = pairs == own_pair
        first_start = jnp.min(jnp.where(same, starts, FAR), axis=1, keepdims=True)
        first_end = jnp.min(jnp.where(same, ends, FAR), axis=1, keepdims=True)
        key_width = 2 * D_HEAD
        parts = seq_len // key_width
        for part in range(parts):
            key_pos = (
                lax.broadcasted_iota(jnp.int32, (tokens, key_width), 1) + part * key_width
            ).astype(jnp.float32)
            seen = (key_pos <= position) & (
                (key_pos >= own_start) | ((key_pos >= first_start) & (key_pos < first_end))
            )
            bias[part] = jnp.where(seen, 0.0, NEGATIVE)

        kv_copy(first, first, 0).wait_recv()

        @pl.when(core == 1)
        def _():
            kv_copy(second, first, 2).start()
            send_queries(1)

        kv_copy(partner, first, 3).start()
        kv_copy(second, second, 1).wait_recv()
        kv_copy(partner, second, 3).start()

        def pass_on(at):
            wz_copy(at).wait_recv()
            relay(at).start()

        def complete(at):
            whole(w_far.at[pl.ds(0, share), tile_cols(at)], near_sems.at[at])

        pass_on(0)
        kv_copy(second, corner, 2).wait_recv()
        kv_copy(partner, corner, 3).start()
        pass_on(1)
        gather_queries(0)
        pass_on(2)
        whole(kv_all.at[:, pl.ds(0, seq_count // 2 * tokens)], kv_sems.at[3])

        scale = math.log2(math.e) / math.sqrt(D_HEAD)

        def unit(group, part, kept):
            rows_q = q_heads[group, part, kept]
            scores = []
            for block in range(parts):
                masks = []
                for kind in range(2):
                    rows_at = (2 * kept + kind) * block_rows
                    masks += [bias[block, rows_at : rows_at + block_rows, :]] * pair_heads
                scores.append(
                    lax.dot_general(
                        rows_q,
                        kv_all[0, block * key_width : (block + 1) * key_width],
                        (((1,), (1,)), ((), ())),
                        preferred_element_type=jnp.float32,
                    )
                    * scale
                    + jnp.concatenate(masks, axis=0)
                )
            top = functools.reduce(jnp.maximum, scores)
            top = jnp.max(top, axis=1, keepdims=True)
            total = jnp.zeros((2 * pair_heads * block_rows, key_width), jnp.float32)
            summed = jnp.zeros((2 * pair_heads * block_rows, D_HEAD), jnp.float32)
            for block in range(parts):
                weights = jnp.exp2(scores[block] - top)
                total = total + weights
                summed = summed + jnp.dot(
                    weights.astype(jnp.bfloat16),
                    kv_all[1, block * key_width : (block + 1) * key_width],
                    preferred_element_type=jnp.float32,
                )
            total = jnp.sum(total, axis=1, keepdims=True)
            result = (summed / total).astype(jnp.bfloat16)
            for kind in range(2):
                for head in range(pair_heads):
                    row = (kind * pair_heads + head) * block_rows
                    at = ((group * 2 + part) * pair_heads + head) * D_HEAD
                    attended[kept, side, core, kind, :, pl.ds(pl.multiple_of(at, D_HEAD), D_HEAD)] = (
                        result[row : row + block_rows]
                    )

        def product(rows_a, at):
            return jnp.dot(
                rows_a[:, :width], w_own[:, tile_cols(at)], preferred_element_type=jnp.float32
            ) + jnp.dot(
                rows_a[:, width:], w_far[:, tile_cols(at)], preferred_element_type=jnp.float32
            )

        def half_term(which):
            rows_a = attended[0, side, which].reshape(2 * block_rows, 2 * width)
            sent[0, core_rows(which)] = product(rows_a, 0).astype(jnp.bfloat16)
            start_copy(which).start()

        def term(kept, half, at):
            return product(attended[kept, half].reshape(rows_all, 2 * width), at)

        def send_term(message):
            at, other = order(message)

            @pl.when(jnp.logical_not(other))
            def _():
                complete(at)

            half = jnp.where(other, 1 - side, side)
            sent[message] = term(0, half, at).astype(jnp.bfloat16)
            b_copy(message).start()

        ends = ((messages - 2, 1 - side), (messages - 1, side))

        def send_last():
            complete(tiles - 1)
            for message, half in ends:
                sent[message] = term(0, half, tiles - 1).astype(jnp.bfloat16)
            for kind in range(2):
                for message, half in ends:
                    for which in range(2):
                        last_copy(message, kind, which).start()

        def keep_last():
            at = tiles - 1
            mixed = [term(1, half, at) for message, half in ends]
            for kind in range(2):
                for part, (message, half) in enumerate(ends):
                    whole(arrived.at[message, core_rows(0)], b_sems.at[message + 2 * kind])
                    for which in range(2):
                        row = (2 * which + kind) * block_rows
                        rows = slice(row, row + block_rows)
                        final[message, rows] = (
                            mixed[part][rows] + arrived[message, rows].astype(jnp.float32)
                        ).astype(jnp.bfloat16)
                        if kind == 0:
                            edge_copy(message, at, half, which).start()
                        elif part == 0:
                            inner_copy(message, at, half, which).start()
            inner_copy(messages - 1, at, side, 1 - core).start()
            out_copy(messages - 1, at).start()

        def keep_term(message):
            at, other = order(message)
            half = jnp.where(other, 1 - side, side)
            mixed = term(1, half, at)
            b_copy(message).wait_recv()
            final[message] = (mixed + arrived[message].astype(jnp.float32)).astype(jnp.bfloat16)
            edge_copy(message, at, half, 0).start()
            edge_copy(message, at, half, 1).start()
            inner_copy(message, at, half, 1 - core).start()

            @pl.when(other)
            def _():
                inner_copy(message, at, half, core).start()

            @pl.when(jnp.logical_not(other))
            def _():
                out_copy(message, at).start()

        def share_out(kept, item):
            a_copy(kept, item, 1, along_x).start()
            a_copy(kept, item, 0, partner).start()

        def wait_rows(kept, kind):
            whole(attended.at[kept, 0, 0], a_sems.at[kept, kind])

        def sent_unit(item, carry):
            @pl.when(item == 1)
            def _():
                gather_queries(1)
                pass_on(3)

            @pl.when(item >= 2)
            def _():
                qz_copy(item - 2, 0).wait_recv()

            unit(item // 2, lax.rem(item, 2), 0)
            share_out(0, item)
            return carry

        def kept_unit(item, carry):
            @pl.when(item >= 2)
            def _():
                qz_copy(item - 2, 1).wait_recv()

            unit(item // 2, lax.rem(item, 2), 1)
            share_out(1, item)
            return carry

        lax.fori_loop(0, 4, sent_unit, 0)
        own_copy.wait()
        pass_on(4)
        complete(0)
        half_term(core)
        wait_rows(0, 0)
        half_term(1 - core)
        pass_on(5)
        lax.fori_loop(0, 2, kept_unit, 0)
        pass_on(6)
        send_term(1)
        wait_rows(0, 1)
        far_copy(0).start()
        pass_on(7)
        wait_rows(0, 2)
        send_term(2)
        send_term(3)
        pass_on(8)
        lax.fori_loop(2, 4, kept_unit, 0)
        pass_on(9)
        send_term(4)
        pass_on(10)
        wait_rows(1, 0)

        def advance(message, carry):
            @pl.when(message + ON < messages)
            def _():
                pass_on(message + ON)

            @pl.when(message + AHEAD < messages - 2)
            def _():
                send_term(message + AHEAD)

            @pl.when(message + AHEAD == messages - 2)
            def _():
                send_last()

            @pl.when(message == 1)
            def _():
                wait_rows(1, 1)
                far_copy(1).start()

            @pl.when(message == 2)
            def _():
                wait_rows(1, 2)

            keep_term(message)
            return carry

        lax.fori_loop(0, messages - 2, advance, 0)
        keep_last()

        whole(final, send_sems.at[10])
        whole(sent, send_sems.at[9])
        whole(attended.at[0], send_sems.at[8])
        whole(attended.at[0, 0], send_sems.at[7])
        whole(w_far.at[pl.ds(0, share)], send_sems.at[5])
        whole(kv_all.at[:, pl.ds(0, (seq_count - 1) * tokens)], send_sems.at[0])
        whole(out_ref.at[:, pl.ds(0, 3 * quarter)], f_sems.at[1])

    whole(q_send.at[:, pl.ds(0, seq_count - 1)], send_sems.at[1])


def fused_device(queries, keys, values, out_weight, doc_lengths, pair_ids, block_plan):
    seq_count = lax.axis_size("seq")
    head_count = lax.axis_size("head")
    tokens, width = queries.shape
    slots = block_plan.shape[0] // seq_count
    block_rows = tokens // slots
    out_width = out_weight.shape[1]
    quarter = out_width // 4
    tiles = pick_tiles(quarter)
    tile = quarter // tiles
    half = jnp.bfloat16
    flow = pltpu.VMEM((2 * tiles, 4 * block_rows, tile), half)
    weights = pltpu.VMEM((width, quarter), half)
    in_vmem = pl.BlockSpec(memory_space=pltpu.VMEM)
    anywhere = pl.BlockSpec(memory_space=pl.ANY)
    in_smem = pl.BlockSpec(memory_space=pltpu.SMEM)
    dma = pltpu.SemaphoreType.DMA
    return pl.pallas_call(
        functools.partial(fused_kernel, seq_count, head_count),
        out_shape=pltpu.VMEM((block_rows, out_width), half),
        in_specs=[anywhere, anywhere, anywhere, anywhere, in_vmem, in_smem, in_smem],
        out_specs=in_vmem,
        scratch_shapes=[
            pltpu.VMEM((slots, block_rows, width), half),
            pltpu.VMEM(keys.shape, half),
            pltpu.VMEM(values.shape, half),
            weights,
            weights,
            pltpu.VMEM((2, seq_count * tokens, D_HEAD), half),
            pltpu.VMEM((2, seq_count, block_rows, width // 2), half),
            pltpu.VMEM((seq_count, block_rows, width // 2), half),
            pltpu.VMEM((seq_count, block_rows, width // 2), half),
            pltpu.VMEM((2, 2, 2, width // D_HEAD * block_rows, D_HEAD), half),
            pltpu.VMEM(
                (seq_count * tokens // (2 * D_HEAD), tokens, 2 * D_HEAD), jnp.float32
            ),
            pltpu.VMEM((2, 2, 2, 2, block_rows, 2 * width), half),
            flow,
            flow,
            flow,
            dma((4,)),
            dma((11,)),
            dma((4,)),
            dma((2,)),
            dma((2, 2)),
            dma((2 * tiles,)),
            dma((tiles,)),
            dma((2, 3)),
            dma((2 * tiles + 2,)),
            dma((2,)),
        ],
        compiler_params=pltpu.CompilerParams(
            collective_id=0, has_side_effects=True, vmem_limit_bytes=60000 * 1024
        ),
    )(
        queries.reshape(slots, block_rows, width),
        keys,
        values,
        out_weight,
        pair_ids[None],
        doc_lengths,
        block_plan,
    )


def pick_device(queries, keys, values, out_weight, doc_lengths, pair_ids, block_plan):
    seq_count = lax.axis_size("seq")
    head_count = lax.axis_size("head")
    tokens, width = queries.shape
    out_width = out_weight.shape[1]
    block_rows = tokens * seq_count // block_plan.shape[0]
    fits = seq_count * tokens * tokens * 4 <= 4 * 1024 * 1024
    shape = head_count == 4 and seq_count == 8 and keys.shape[1] == 2 * D_HEAD and width % (2 * D_HEAD) == 0
    square = block_rows * head_count == tokens and block_rows % 16 == 0
    even = seq_count * tokens % (2 * D_HEAD) == 0 and width % 64 == 0
    wide = out_width % 2 == 0 and out_width // 4 % (8 * 128) == 0
    run = fused_device if fits and shape and square and even and wide else on_device
    return run(queries, keys, values, out_weight, doc_lengths, pair_ids, block_plan)


def solution(mesh):
    return jax.shard_map(
        pick_device,
        mesh=mesh,
        in_specs=(P("seq", "head"), P("seq", None), P("seq", None), P("head", None), P(), P(), P()),
        out_specs=P(("seq", "head"), None),
        check_vma=False,
    )
```

```python
import functools
import math

import jax
import jax.numpy as jnp
from jax import lax
from jax.experimental import pallas as pl
from jax.experimental.pallas import tpu as pltpu
from jax.sharding import PartitionSpec as P

D_HEAD = 128


NEGATIVE = -1e30


def token_docs(positions, doc_lengths):
    doc_ends = jnp.cumsum(doc_lengths)
    return jnp.sum((doc_ends[None, :] <= positions[:, None]).astype(jnp.int32), axis=1)


def pair_firsts(docs, pair_ids):
    doc_range = jnp.arange(pair_ids.shape[0], dtype=jnp.int32)
    own_pair = jnp.sum(jnp.where(docs[:, None] == doc_range[None, :], pair_ids[None, :], 0), axis=1)
    return jnp.sum((pair_ids[None, :] < own_pair[:, None]).astype(jnp.int32), axis=1)


def largest_divisor(total_rows, ceiling):
    return max(
        (
            candidate
            for candidate in range(1, min(total_rows, ceiling) + 1)
            if total_rows % candidate == 0
        )
    )


def attend(query_rows, positions, keys, values, doc_lengths, pair_ids):
    head_size = keys.shape[1]
    token_count = query_rows.shape[0]
    query_heads = query_rows.shape[1] // head_size
    shaped_queries = query_rows.reshape(token_count, query_heads, head_size)
    query_docs = token_docs(positions, doc_lengths)
    query_firsts = pair_firsts(query_docs, pair_ids)
    doc_range = jnp.arange(doc_lengths.shape[0], dtype=jnp.int32)
    pair_begin = jnp.sum(
        jnp.where(doc_range[None, :] < query_firsts[:, None], doc_lengths[None, :], 0), axis=1
    )
    lowest = jnp.min(pair_begin)
    highest = jnp.max(positions)
    scale = 1.0 / math.sqrt(head_size)

    def update(softmax_state, key_block, value_block, block_start):
        key_pos = block_start + jnp.arange(key_block.shape[0], dtype=jnp.int32)
        needed = (block_start <= highest) & (block_start + key_block.shape[0] > lowest)

        def compute(current):
            running_max, denominator, weighted = current
            key_docs = token_docs(key_pos, doc_lengths)
            allowed = (key_pos[None, :] <= positions[:, None]) & (
                (key_docs[None, :] == query_docs[:, None])
                | (key_docs[None, :] == query_firsts[:, None])
            )
            scores = (
                jnp.einsum(
                    "qhd,kd->hqk", shaped_queries, key_block, preferred_element_type=jnp.float32
                )
                * scale
            )
            newest = jnp.maximum(
                running_max, jnp.max(jnp.where(allowed[None], scores, NEGATIVE), axis=2)
            )
            weights = jnp.where(allowed[None], jnp.exp(scores - newest[:, :, None]), 0.0)
            factor = jnp.exp(running_max - newest)
            denominator = denominator * factor + jnp.sum(weights, axis=2)
            weighted = weighted * factor[:, :, None] + jnp.einsum(
                "hqk,kd->hqd",
                weights.astype(jnp.bfloat16),
                value_block,
                preferred_element_type=jnp.float32,
            )
            return (newest, denominator, weighted)

        def unchanged(current):
            return current

        return lax.cond(needed, compute, unchanged, softmax_state)

    initial = (
        jnp.full((query_heads, token_count), NEGATIVE, jnp.float32),
        jnp.zeros((query_heads, token_count), jnp.float32),
        jnp.zeros((query_heads, token_count, head_size), jnp.float32),
    )
    key_rows = lax.all_gather(keys, "seq", axis=0, tiled=True)
    value_rows = lax.all_gather(values, "seq", axis=0, tiled=True)
    row_total = key_rows.shape[0]
    block_rows = largest_divisor(row_total, 1024)
    block_count = row_total // block_rows
    stacked = (
        key_rows.reshape(block_count, block_rows, head_size),
        value_rows.reshape(block_count, block_rows, head_size),
        jnp.int32(0) + block_rows * jnp.arange(block_count, dtype=jnp.int32),
    )

    def advance(carried, block_item):
        return (update(carried, block_item[0], block_item[1], block_item[2]), None)

    result_state, unused_out = lax.scan(advance, initial, stacked)
    running_max, denominator, weighted = result_state
    attended = weighted / denominator[:, :, None]
    return (
        attended.transpose(1, 0, 2)
        .reshape(token_count, query_heads * head_size)
        .astype(jnp.bfloat16)
    )


def on_device(queries, keys, values, out_weight, doc_lengths, pair_ids, block_plan):
    seq_count = lax.axis_size("seq")
    my_seq = lax.axis_index("seq")
    shared_head = lax.axis_index("head") // 2
    key_rows = lax.dynamic_slice_in_dim(keys, shared_head * D_HEAD, D_HEAD, 1)
    value_rows = lax.dynamic_slice_in_dim(values, shared_head * D_HEAD, D_HEAD, 1)
    slots_here = seq_count // 2
    tok_rows = queries.shape[0]
    row_width = queries.shape[1]
    block_rows = tok_rows // slots_here
    slot_total = block_plan.shape[0]
    local_ids = my_seq * slots_here + jnp.arange(slots_here, dtype=jnp.int32)
    plan_rows = lax.dynamic_slice_in_dim(block_plan, my_seq * slots_here, slots_here, 0)
    planned_pos = (
        plan_rows[:, None] * block_rows + jnp.arange(block_rows, dtype=jnp.int32)[None, :]
    ).reshape(-1)
    slot_range = jnp.arange(slot_total, dtype=jnp.int32)
    target_slot = jnp.sum(
        jnp.where(block_plan[None, :] == local_ids[:, None], slot_range[None, :], 0), axis=1
    )
    device_range = jnp.arange(seq_count, dtype=jnp.int32)
    send_table = ((target_slot // slots_here)[:, None] == device_range[None, :]).astype(
        jnp.bfloat16
    )
    take_table = ((plan_rows // slots_here)[:, None] == device_range[None, :]).astype(jnp.bfloat16)
    blocked = queries.reshape(slots_here, block_rows, row_width)
    arrived = lax.all_to_all(
        jnp.einsum("bn,bkw->nkw", send_table, blocked, preferred_element_type=jnp.float32).astype(
            jnp.bfloat16
        ),
        "seq",
        split_axis=0,
        concat_axis=0,
        tiled=True,
    )
    chosen = jnp.einsum("bn,nkw->bkw", take_table, arrived, preferred_element_type=jnp.float32)
    attended = attend(
        chosen.astype(jnp.bfloat16).reshape(tok_rows, row_width),
        planned_pos,
        key_rows,
        value_rows,
        doc_lengths,
        pair_ids,
    )
    return lax.psum_scatter(
        jnp.dot(attended, out_weight, preferred_element_type=jnp.float32).astype(jnp.bfloat16),
        "head",
        scatter_dimension=0,
        tiled=True,
    )


FAR = 1e9
AHEAD = 5
EARLY = 4
ON = 10


def pick_tiles(width):
    return max(c for c in (1, 2, 4, 8) if width % (c * 128) == 0)


def fused_kernel(
    seq_count,
    head_count,
    queries_hbm,
    keys_hbm,
    values_hbm,
    weight_hbm,
    pairs_ref,
    lens_ref,
    plan_ref,
    out_ref,
    queries_ref,
    w_own,
    w_far,
    kv_all,
    q_send,
    q_recv_a,
    q_recv_b,
    q_heads,
    bias,
    attended,
    sent,
    arrived,
    final,
    load_sems,
    send_sems,
    kv_sems,
    q_sems,
    qz_sems,
    wz_sems,
    near_sems,
    a_sems,
    b_sems,
    f_sems,
):
    q_recv = (q_recv_a, q_recv_b)
    me = lax.axis_index("seq")
    rank = lax.axis_index("head")
    core = lax.rem(me, 2)
    partner = me + 1 - 2 * core
    along_x = me + 2 - 4 * lax.rem(me // 2, 2)
    along_y = lax.rem(me + seq_count // 2, seq_count)
    first = along_y
    second = along_x
    corner = along_x + along_y - me
    quad = lax.rem(me, 4)
    base = me - quad
    side = quad // 2
    low = rank < head_count // 2
    inner = (rank > 0) & (rank < head_count - 1)
    mate = rank + 1 - 2 * lax.rem(rank, 2)
    across = head_count - 1 - rank
    slots, block_rows, width = queries_ref.shape
    tokens = slots * block_rows
    seq_len = seq_count * tokens
    pair_heads = width // (2 * D_HEAD)
    pair_width = pair_heads * D_HEAD
    shared = head_count // (keys_hbm.shape[1] // D_HEAD)
    messages, rows_all, tile = sent.shape
    tiles = messages // 2
    quarter = tiles * tile
    share = width // (seq_count // 4)
    piece = share // 2

    def slot_at(place):
        at = (head_count - 1, head_count // 2, 0, 1)[place]
        return jnp.where(low, at, head_count - 1 - at)

    def piece_rows(device, at):
        return pl.ds(
            pl.multiple_of((device // 4) * share + lax.rem(at, 2) * piece, piece), piece
        )

    def tile_cols(at):
        return pl.ds(pl.multiple_of(at * tile, tile), tile)

    def out_cols(owner, at):
        return pl.ds(pl.multiple_of(owner * quarter + at * tile, tile), tile)

    def order(message):
        message = jnp.int32(message)
        late = message == messages - 3
        odd = lax.rem(message, 2) == 1
        other = late | ((message >= 2) & jnp.logical_not(odd))
        at = jnp.where(odd, (message + 1) // 2, (message - 2) // 2)
        at = jnp.where(late, tiles - 2, jnp.where(message == 0, 0, at))
        return at, other

    own_copy = pltpu.make_async_copy(
        weight_hbm.at[:, pl.ds(pl.multiple_of(quad * quarter, quarter), quarter)],
        w_own,
        load_sems.at[0],
    )
    queries_copy = pltpu.make_async_copy(queries_hbm, queries_ref, load_sems.at[1])
    kv_col = pl.ds(pl.multiple_of((rank // shared) * D_HEAD, D_HEAD), D_HEAD)
    mine = pl.ds(pl.multiple_of(me * tokens, tokens), tokens)
    keys_copy = pltpu.make_async_copy(
        keys_hbm.at[:, kv_col], kv_all.at[0, mine], load_sems.at[2]
    )
    values_copy = pltpu.make_async_copy(
        values_hbm.at[:, kv_col], kv_all.at[1, mine], load_sems.at[3]
    )

    barrier = pltpu.get_barrier_semaphore()
    for step in range(1, seq_count):
        pl.semaphore_signal(barrier, inc=1, device_id={"seq": lax.rem(me + step, seq_count)})

    for place in range(4):
        pl.semaphore_signal(barrier, inc=1, device_id={"seq": base + place, "head": mate})

    @pl.when(inner)
    def _():
        pl.semaphore_signal(barrier, inc=1, device_id={"head": across})

    @pl.when(inner)
    def _():
        keys_copy.start()
        values_copy.start()

    queries_copy.start()

    @pl.when(inner)
    def _():
        keys_copy.wait()
        values_copy.wait()

    def sort_queries():
        queries_copy.wait()
        for other in range(seq_count):
            local = jnp.int32(0)
            for slot in range(slots):
                offset = plan_ref[other * slots + slot] - me * slots
                local = local + jnp.where((offset >= 0) & (offset < slots), offset, 0)
            block = queries_ref[local]
            for part in range(2):
                q_send[part, other] = block[:, part * pair_width : (part + 1) * pair_width]
        for part in range(2):
            q_recv[part][me] = q_send[part, me]

    @pl.when(jnp.logical_not(inner))
    def _():
        sort_queries()

    pl.semaphore_wait(barrier, seq_count + 3 + jnp.where(inner, 1, 0))

    def kv_copy(peer, slot, sem):
        rows = pl.ds(pl.multiple_of(slot * tokens, tokens), tokens)
        return pltpu.make_async_remote_copy(
            src_ref=kv_all.at[:, rows],
            dst_ref=kv_all.at[:, rows],
            send_sem=send_sems.at[0],
            recv_sem=kv_sems.at[sem],
            device_id={"seq": peer},
        )

    def q_copy(part, peer, slot):
        return pltpu.make_async_remote_copy(
            src_ref=q_send.at[part, peer],
            dst_ref=q_recv[part].at[slot],
            send_sem=send_sems.at[1],
            recv_sem=q_sems.at[part],
            device_id={"seq": peer},
        )

    def qz_copy(part, kept):
        return pltpu.make_async_remote_copy(
            src_ref=q_heads.at[0, part, kept],
            dst_ref=q_heads.at[1, part, kept],
            send_sem=send_sems.at[2],
            recv_sem=qz_sems.at[part, kept],
            device_id={"head": mate},
        )

    def wz_copy(at):
        rows = piece_rows(me, at)
        return pltpu.make_async_remote_copy(
            src_ref=weight_hbm.at[rows, out_cols(quad, at // 2)],
            dst_ref=w_far.at[rows, tile_cols(at // 2)],
            send_sem=send_sems.at[3],
            recv_sem=wz_sems.at[at],
            device_id={"head": mate},
        )

    def relay(at):
        rows = piece_rows(me, at)
        return pltpu.make_async_remote_copy(
            src_ref=w_far.at[rows, tile_cols(at // 2)],
            dst_ref=w_far.at[rows, tile_cols(at // 2)],
            send_sem=send_sems.at[5],
            recv_sem=near_sems.at[at // 2],
            device_id={"seq": along_y},
        )

    def a_copy(kept, item, kind, peer):
        cols = pl.ds(pl.multiple_of(item * pair_width, pair_width), pair_width)
        return pltpu.make_async_remote_copy(
            src_ref=attended.at[kept, side, core, :, :, cols],
            dst_ref=attended.at[kept, side, core, :, :, cols],
            send_sem=send_sems.at[8],
            recv_sem=a_sems.at[kept, kind],
            device_id={"seq": peer},
        )

    def far_copy(kept):
        return pltpu.make_async_remote_copy(
            src_ref=attended.at[kept, 1 - side, core],
            dst_ref=attended.at[kept, 1 - side, core],
            send_sem=send_sems.at[7],
            recv_sem=a_sems.at[kept, 2],
            device_id={"seq": partner},
        )

    def core_rows(which):
        return pl.ds(pl.multiple_of(which * 2 * block_rows, block_rows), 2 * block_rows)

    def start_copy(which):
        return pltpu.make_async_remote_copy(
            src_ref=sent.at[0, core_rows(which)],
            dst_ref=arrived.at[0, core_rows(which)],
            send_sem=send_sems.at[9],
            recv_sem=b_sems.at[0],
            device_id={"head": across},
        )

    def b_copy(at):
        return pltpu.make_async_remote_copy(
            src_ref=sent.at[at],
            dst_ref=arrived.at[at],
            send_sem=send_sems.at[9],
            recv_sem=b_sems.at[at],
            device_id={"head": across},
        )

    def kind_rows(which, kind):
        return pl.ds(pl.multiple_of((2 * which + kind) * block_rows, block_rows), block_rows)

    def last_copy(message, kind, which):
        row = (2 * which + kind) * block_rows
        rows = pl.ds(row, block_rows)
        return pltpu.make_async_remote_copy(
            src_ref=sent.at[message, rows],
            dst_ref=arrived.at[message, rows],
            send_sem=send_sems.at[9],
            recv_sem=b_sems.at[message + 2 * kind],
            device_id={"head": across},
        )

    def edge_copy(message, at, half, which):
        return pltpu.make_async_remote_copy(
            src_ref=final.at[message, kind_rows(which, 0)],
            dst_ref=out_ref.at[:, out_cols(quad, at)],
            send_sem=send_sems.at[10],
            recv_sem=f_sems.at[0],
            device_id={"seq": base + 2 * half + which, "head": mate},
        )

    def inner_copy(message, at, half, which):
        return pltpu.make_async_remote_copy(
            src_ref=final.at[message, kind_rows(which, 1)],
            dst_ref=out_ref.at[:, out_cols(quad, at)],
            send_sem=send_sems.at[10],
            recv_sem=f_sems.at[1],
            device_id={"seq": base + 2 * half + which},
        )

    def out_copy(message, at):
        return pltpu.make_async_copy(
            final.at[message, kind_rows(core, 1)],
            out_ref.at[:, out_cols(quad, at)],
            send_sems.at[10],
        )

    def whole(ref, sem):
        pltpu.make_async_copy(ref, ref, sem).wait()

    @pl.when(inner)
    def _():
        kv_copy(first, me, 0).start()
        kv_copy(second, me, 1).start()
        kv_copy(partner, me, 3).start()

        @pl.when(core == 0)
        def _():
            kv_copy(corner, me, 2).start()

        own_copy.start()
        sort_queries()

    @pl.when(jnp.logical_not(inner))
    def _():
        for at in range(EARLY):
            wz_copy(at).start()

    def send_queries(part):
        for step in range(1, seq_count):
            peer = lax.rem(me + step, seq_count)
            q_copy(part, peer, me).start()

    send_queries(0)

    @pl.when(jnp.logical_not(inner) | (core == 0))
    def _():
        send_queries(1)

    def gather_queries(part):
        whole(q_recv[part].at[pl.ds(0, seq_count - 1)], q_sems.at[part])
        for place in range(slots):
            block = q_recv[part][plan_ref[me * slots + slot_at(place)] // slots]
            for head in range(pair_heads):
                row = ((place % 2) * pair_heads + head) * block_rows
                q_heads[0, part, place // 2, row : row + block_rows, :] = block[
                    :, head * D_HEAD : (head + 1) * D_HEAD
                ]

    @pl.when(jnp.logical_not(inner))
    def _():
        gather_queries(0)
        qz_copy(0, 0).start()
        gather_queries(1)
        qz_copy(1, 0).start()
        for at in range(EARLY, EARLY + 4):
            wz_copy(at).start()
        qz_copy(0, 1).start()
        qz_copy(1, 1).start()

        def push_next(at, carry):
            wz_copy(at).start()
            return carry

        lax.fori_loop(EARLY + 4, messages, push_next, 0)
        whole(out_ref, f_sems.at[0])
        whole(weight_hbm.at[pl.ds(0, share), pl.ds(0, quarter)], send_sems.at[3])
        whole(q_heads.at[0], send_sems.at[2])

    @pl.when(inner)
    def _():
        row = lax.broadcasted_iota(jnp.int32, (tokens, 1), 0)
        position = row
        for place in range(slots):
            shift = (plan_ref[me * slots + slot_at(place)] - place) * block_rows
            here = (row >= place * block_rows) & (row < (place + 1) * block_rows)
            position = position + jnp.where(here, shift, 0)
        position = position.astype(jnp.float32)
        docs = pairs_ref.shape[1]
        doc_at = lax.broadcasted_iota(jnp.int32, (1, docs), 1)
        starts = jnp.zeros((1, docs), jnp.int32)
        ends = jnp.zeros((1, docs), jnp.int32)
        running = jnp.int32(0)
        for doc in range(docs):
            starts = jnp.where(doc_at == doc, running, starts)
            running = running + lens_ref[doc]
            ends = jnp.where(doc_at == doc, running, ends)
        starts = starts.astype(jnp.float32)
        ends = ends.astype(jnp.float32)
        pairs = pairs_ref[...].astype(jnp.float32)
        begun = starts <= position
        own_start = jnp.max(jnp.where(begun, starts, 0.0), axis=1, keepdims=True)
        own_pair = jnp.max(jnp.where(begun, pairs, 0.0), axis=1, keepdims=True)
        same = pairs == own_pair
        first_start = jnp.min(jnp.where(same, starts, FAR), axis=1, keepdims=True)
        first_end = jnp.min(jnp.where(same, ends, FAR), axis=1, keepdims=True)
        key_width = 2 * D_HEAD
        parts = seq_len // key_width
        for part in range(parts):
            key_pos = (
                lax.broadcasted_iota(jnp.int32, (tokens, key_width), 1) + part * key_width
            ).astype(jnp.float32)
            seen = (key_pos <= position) & (
                (key_pos >= own_start) | ((key_pos >= first_start) & (key_pos < first_end))
            )
            bias[part] = jnp.where(seen, 0.0, NEGATIVE)

        kv_copy(first, first, 0).wait_recv()

        @pl.when(core == 1)
        def _():
            kv_copy(second, first, 2).start()
            send_queries(1)

        kv_copy(partner, first, 3).start()
        kv_copy(second, second, 1).wait_recv()
        kv_copy(partner, second, 3).start()

        def pass_on(at):
            wz_copy(at).wait_recv()
            relay(at).start()

        def complete(at):
            whole(w_far.at[pl.ds(0, share), tile_cols(at)], near_sems.at[at])

        pass_on(0)
        kv_copy(second, corner, 2).wait_recv()
        kv_copy(partner, corner, 3).start()
        pass_on(1)
        gather_queries(0)
        pass_on(2)
        whole(kv_all.at[:, pl.ds(0, seq_count // 2 * tokens)], kv_sems.at[3])

        scale = math.log2(math.e) / math.sqrt(D_HEAD)

        def unit(group, part, kept):
            rows_q = q_heads[group, part, kept]
            scores = []
            for block in range(parts):
                masks = []
                for kind in range(2):
                    rows_at = (2 * kept + kind) * block_rows
                    masks += [bias[block, rows_at : rows_at + block_rows, :]] * pair_heads
                scores.append(
                    lax.dot_general(
                        rows_q,
                        kv_all[0, block * key_width : (block + 1) * key_width],
                        (((1,), (1,)), ((), ())),
                        preferred_element_type=jnp.float32,
                    )
                    * scale
                    + jnp.concatenate(masks, axis=0)
                )
            top = functools.reduce(jnp.maximum, scores)
            top = jnp.max(top, axis=1, keepdims=True)
            total = jnp.zeros((2 * pair_heads * block_rows, key_width), jnp.float32)
            summed = jnp.zeros((2 * pair_heads * block_rows, D_HEAD), jnp.float32)
            for block in range(parts):
                weights = jnp.exp2(scores[block] - top)
                total = total + weights
                summed = summed + jnp.dot(
                    weights.astype(jnp.bfloat16),
                    kv_all[1, block * key_width : (block + 1) * key_width],
                    preferred_element_type=jnp.float32,
                )
            total = jnp.sum(total, axis=1, keepdims=True)
            result = (summed / total).astype(jnp.bfloat16)
            for kind in range(2):
                for head in range(pair_heads):
                    row = (kind * pair_heads + head) * block_rows
                    at = ((group * 2 + part) * pair_heads + head) * D_HEAD
                    attended[kept, side, core, kind, :, pl.ds(pl.multiple_of(at, D_HEAD), D_HEAD)] = (
                        result[row : row + block_rows]
                    )

        def product(rows_a, at):
            return jnp.dot(
                rows_a[:, :width], w_own[:, tile_cols(at)], preferred_element_type=jnp.float32
            ) + jnp.dot(
                rows_a[:, width:], w_far[:, tile_cols(at)], preferred_element_type=jnp.float32
            )

        def half_term(which):
            rows_a = attended[0, side, which].reshape(2 * block_rows, 2 * width)
            sent[0, core_rows(which)] = product(rows_a, 0).astype(jnp.bfloat16)
            start_copy(which).start()

        def term(kept, half, at):
            return product(attended[kept, half].reshape(rows_all, 2 * width), at)

        def send_term(message):
            at, other = order(message)

            @pl.when(jnp.logical_not(other))
            def _():
                complete(at)

            half = jnp.where(other, 1 - side, side)
            sent[message] = term(0, half, at).astype(jnp.bfloat16)
            b_copy(message).start()

        ends = ((messages - 2, 1 - side), (messages - 1, side))

        def send_last():
            complete(tiles - 1)
            for message, half in ends:
                sent[message] = term(0, half, tiles - 1).astype(jnp.bfloat16)
            for kind in range(2):
                for message, half in ends:
                    for which in range(2):
                        last_copy(message, kind, which).start()

        def keep_last():
            at = tiles - 1
            mixed = [term(1, half, at) for message, half in ends]
            for kind in range(2):
                for part, (message, half) in enumerate(ends):
                    whole(arrived.at[message, core_rows(0)], b_sems.at[message + 2 * kind])
                    for which in range(2):
                        row = (2 * which + kind) * block_rows
                        rows = slice(row, row + block_rows)
                        final[message, rows] = (
                            mixed[part][rows] + arrived[message, rows].astype(jnp.float32)
                        ).astype(jnp.bfloat16)
                        if kind == 0:
                            edge_copy(message, at, half, which).start()
                        elif part == 0:
                            inner_copy(message, at, half, which).start()
            inner_copy(messages - 1, at, side, 1 - core).start()
            out_copy(messages - 1, at).start()

        def keep_term(message):
            at, other = order(message)
            half = jnp.where(other, 1 - side, side)
            mixed = term(1, half, at)
            b_copy(message).wait_recv()
            final[message] = (mixed + arrived[message].astype(jnp.float32)).astype(jnp.bfloat16)
            edge_copy(message, at, half, 0).start()
            edge_copy(message, at, half, 1).start()
            inner_copy(message, at, half, 1 - core).start()

            @pl.when(other)
            def _():
                inner_copy(message, at, half, core).start()

            @pl.when(jnp.logical_not(other))
            def _():
                out_copy(message, at).start()

        def share_out(kept, item):
            a_copy(kept, item, 1, along_x).start()
            a_copy(kept, item, 0, partner).start()

        def wait_rows(kept, kind):
            whole(attended.at[kept, 0, 0], a_sems.at[kept, kind])

        def sent_unit(item, carry):
            @pl.when(item == 1)
            def _():
                gather_queries(1)
                pass_on(3)

            @pl.when(item >= 2)
            def _():
                qz_copy(item - 2, 0).wait_recv()

            unit(item // 2, lax.rem(item, 2), 0)
            share_out(0, item)
            return carry

        def kept_unit(item, carry):
            @pl.when(item >= 2)
            def _():
                qz_copy(item - 2, 1).wait_recv()

            unit(item // 2, lax.rem(item, 2), 1)
            share_out(1, item)
            return carry

        lax.fori_loop(0, 4, sent_unit, 0)
        own_copy.wait()
        pass_on(4)
        complete(0)
        half_term(core)
        wait_rows(0, 0)
        half_term(1 - core)
        pass_on(5)
        lax.fori_loop(0, 2, kept_unit, 0)
        pass_on(6)
        send_term(1)
        wait_rows(0, 1)
        far_copy(0).start()
        pass_on(7)
        wait_rows(0, 2)
        send_term(2)
        send_term(3)
        pass_on(8)
        lax.fori_loop(2, 4, kept_unit, 0)
        pass_on(9)
        send_term(4)
        wait_rows(1, 0)

        def advance(message, carry):
            @pl.when(message + ON < messages)
            def _():
                pass_on(message + ON)

            @pl.when(message + AHEAD < messages - 2)
            def _():
                send_term(message + AHEAD)

            @pl.when(message + AHEAD == messages - 2)
            def _():
                send_last()

            @pl.when(message == 1)
            def _():
                wait_rows(1, 1)
                far_copy(1).start()

            @pl.when(message == 2)
            def _():
                wait_rows(1, 2)

            keep_term(message)
            return carry

        lax.fori_loop(0, messages - 2, advance, 0)
        keep_last()

        whole(final, send_sems.at[10])
        whole(sent, send_sems.at[9])
        whole(attended.at[0], send_sems.at[8])
        whole(attended.at[0, 0], send_sems.at[7])
        whole(w_far.at[pl.ds(0, share)], send_sems.at[5])
        whole(kv_all.at[:, pl.ds(0, (seq_count - 1) * tokens)], send_sems.at[0])
        whole(out_ref.at[:, pl.ds(0, 3 * quarter)], f_sems.at[1])

    whole(q_send.at[:, pl.ds(0, seq_count - 1)], send_sems.at[1])


def fused_device(queries, keys, values, out_weight, doc_lengths, pair_ids, block_plan):
    seq_count = lax.axis_size("seq")
    head_count = lax.axis_size("head")
    tokens, width = queries.shape
    slots = block_plan.shape[0] // seq_count
    block_rows = tokens // slots
    out_width = out_weight.shape[1]
    quarter = out_width // 4
    tiles = pick_tiles(quarter)
    tile = quarter // tiles
    half = jnp.bfloat16
    flow = pltpu.VMEM((2 * tiles, 4 * block_rows, tile), half)
    weights = pltpu.VMEM((width, quarter), half)
    in_vmem = pl.BlockSpec(memory_space=pltpu.VMEM)
    anywhere = pl.BlockSpec(memory_space=pl.ANY)
    in_smem = pl.BlockSpec(memory_space=pltpu.SMEM)
    dma = pltpu.SemaphoreType.DMA
    return pl.pallas_call(
        functools.partial(fused_kernel, seq_count, head_count),
        out_shape=pltpu.VMEM((block_rows, out_width), half),
        in_specs=[anywhere, anywhere, anywhere, anywhere, in_vmem, in_smem, in_smem],
        out_specs=in_vmem,
        scratch_shapes=[
            pltpu.VMEM((slots, block_rows, width), half),
            weights,
            weights,
            pltpu.VMEM((2, seq_count * tokens, D_HEAD), half),
            pltpu.VMEM((2, seq_count, block_rows, width // 2), half),
            pltpu.VMEM((seq_count, block_rows, width // 2), half),
            pltpu.VMEM((seq_count, block_rows, width // 2), half),
            pltpu.VMEM((2, 2, 2, width // D_HEAD * block_rows, D_HEAD), half),
            pltpu.VMEM(
                (seq_count * tokens // (2 * D_HEAD), tokens, 2 * D_HEAD), jnp.float32
            ),
            pltpu.VMEM((2, 2, 2, 2, block_rows, 2 * width), half),
            flow,
            flow,
            flow,
            dma((4,)),
            dma((11,)),
            dma((4,)),
            dma((2,)),
            dma((2, 2)),
            dma((2 * tiles,)),
            dma((tiles,)),
            dma((2, 3)),
            dma((2 * tiles + 2,)),
            dma((2,)),
        ],
        compiler_params=pltpu.CompilerParams(
            collective_id=0, has_side_effects=True, vmem_limit_bytes=60000 * 1024
        ),
    )(
        queries.reshape(slots, block_rows, width),
        keys,
        values,
        out_weight,
        pair_ids[None],
        doc_lengths,
        block_plan,
    )


def pick_device(queries, keys, values, out_weight, doc_lengths, pair_ids, block_plan):
    seq_count = lax.axis_size("seq")
    head_count = lax.axis_size("head")
    tokens, width = queries.shape
    out_width = out_weight.shape[1]
    block_rows = tokens * seq_count // block_plan.shape[0]
    fits = seq_count * tokens * tokens * 4 <= 4 * 1024 * 1024
    shape = head_count == 4 and seq_count == 8 and keys.shape[1] == 2 * D_HEAD and width % (2 * D_HEAD) == 0
    square = block_rows * head_count == tokens and block_rows % 16 == 0
    even = seq_count * tokens % (2 * D_HEAD) == 0 and width % 64 == 0
    wide = out_width % 2 == 0 and out_width // 4 % (8 * 128) == 0
    run = fused_device if fits and shape and square and even and wide else on_device
    return run(queries, keys, values, out_weight, doc_lengths, pair_ids, block_plan)


def solution(mesh):
    return jax.shard_map(
        pick_device,
        mesh=mesh,
        in_specs=(P("seq", "head"), P("seq", None), P("seq", None), P("head", None), P(), P(), P()),
        out_specs=P(("seq", "head"), None),
        check_vma=False,
    )
```
